128 devices in a mesh: gx: 8 (over z, core), gy: 16 (over y, x).
Axes of the slice: x: 4, y: 4, z: 4, core: 2. Of those that a mesh axis runs over, the one named last changes fastest.
Arguments:
- particles: bfloat16 [64, 256, 64, 256], P('gx', 'gy'), may hold values from -6 to 6
- bias: float32 [64, 256, 64], P('gx', 'gy'), may hold values from -4 to 4
- spread: float32 [64, 256], P('gx', 'gy'), may hold values from 128 to 512
- precision: bfloat16 [64, 64], replicated, may hold values from -1 to 1
- coupling_h: bfloat16 [64, 64], replicated, may hold values from -0.059814453 to 0.059814453
- coupling_v: bfloat16 [64, 64], replicated, may hold values from -0.059814453 to 0.059814453
Outputs:
- force: bfloat16 [64, 256, 64, 256], P('gx', 'gy')
- stein: float32 [], replicated
The draws below stay inside these ranges and needn't reach their ends.
All inputs are finite; a program needn't handle non-finite values.
Results may differ from the reference program's by a relative error of at most 0.0029.
Values may be sent and summed in bfloat16 or wider, within the bound.
A program may use at most 384 MiB of HBM per device.

```python
import math
import jax
import jax.numpy as jnp
from jax import lax

STATE = 64
PARTICLES = 256
NROWS = 64
NCOLS = 256


def draw_precision(key, part):
    first_key, second_key = jax.random.split(jax.random.fold_in(key, 17))
    diagonal = jnp.exp(jax.random.uniform(first_key, (STATE,), jnp.float32, jnp.log(0.2), jnp.log(0.6)))
    raw_values = jax.random.normal(second_key, (STATE, STATE), jnp.float32)
    symmetric = (raw_values + raw_values.T) * (0.07 / STATE ** 0.5)
    return (jnp.diag(diagonal) + symmetric).astype(jnp.bfloat16)


def level_of(key, shape, cuts, least, top_value):
    factor_of, own = 1.0, jax.random.fold_in(key, 6)
    for position, blocks in cuts:
        draws = jnp.exp(jax.random.uniform(jax.random.fold_in(own, position), (blocks,), jnp.float32, least / len(cuts), top_value / len(cuts)))
        factor_of = factor_of * jnp.repeat(draws, shape[position] // blocks).reshape([-1 if axis == position else 1 for axis in range(len(shape))])
    return factor_of


def bell_draw(rng, extent, scale, limit, cuts=(), kind=jnp.bfloat16):
    drawn = jax.random.normal(rng, extent, jnp.float32) * scale
    if len(cuts) > 0:
        drawn = level_of(rng, extent, cuts, -0.22, 0.18) * drawn
    return jnp.clip(drawn, min=-limit, max=limit).astype(kind)


def setup_inputs(seed: int = 0) -> dict:
    key_list = jax.random.split(jax.random.key(seed), 7)
    return {
        "particles": bell_draw(key_list[0], (NROWS, NCOLS, STATE, PARTICLES), 1.0, 6.0, ((0, 8), (1, 16))),
        "bias": bell_draw(key_list[1], (NROWS, NCOLS, STATE), 0.5, 4.0, ((0, 8), (1, 16)), jnp.float32),
        "spread": jnp.clip(jnp.exp(math.log(512.0) - 1.3862944 * jax.random.uniform(key_list[2], (NROWS, NCOLS), jnp.float32) ** level_of(key_list[2], (NROWS, NCOLS), ((0, 8), (1, 16)), -0.2, 0.2)), 128.0, 512.0),
        "precision": draw_precision(jax.random.fold_in(key_list[6], 71), 0),
        "coupling_h": bell_draw(key_list[4], (STATE, STATE), 0.01, 0.059814453),
        "coupling_v": bell_draw(key_list[5], (STATE, STATE), 0.01, 0.059814453),
    }


def distances(states):
    values = states.astype(jnp.float32)
    squares = jnp.sum(values * values, axis=-2)
    inner_prod = jnp.einsum("rcdp,rcdq->rcpq", values, values)
    return squares[..., :, None] + squares[..., None, :] - 2.0 * inner_prod


def mixing(matrix, states):
    return jnp.einsum("ed,rcdp->rcep", matrix.astype(jnp.float32), states.astype(jnp.float32))


def mixing_t(matrix, states):
    return jnp.einsum("de,rcdp->rcep", matrix.astype(jnp.float32), states.astype(jnp.float32))


def finish(states, scores, blanket, own_dist, band):
    band_width = band[..., None, None]
    kernel = jnp.exp(-blanket / band_width)
    kernel_low = kernel.astype(jnp.bfloat16)
    score_low = scores.astype(jnp.bfloat16)
    colsum = jnp.sum(kernel, axis=-2)
    rowsum = jnp.sum(kernel, axis=-1)
    kernel_f = kernel_low.astype(jnp.float32)
    score_f = score_low.astype(jnp.float32)
    states_f = states.astype(jnp.float32)
    pull_sum = jnp.einsum("rcej,rcji->rcei", score_f, kernel_f)
    push_sum = jnp.einsum("rcej,rcji->rcei", states_f, kernel_f)
    inverse_width = 2.0 / band_width
    force = (pull_sum - inverse_width * (push_sum - states_f * colsum[:, :, None, :])).astype(jnp.bfloat16)
    self_dots = jnp.sum(states_f * score_f, axis=-2)
    factor = 2.0 / band
    cross_terms = jnp.sum(score_f * pull_sum, axis=(-2, -1)) + factor * (
        jnp.sum(rowsum * self_dots, axis=-1) - jnp.sum(states_f * pull_sum, axis=(-2, -1))
        - jnp.sum(score_f * push_sum, axis=(-2, -1)) + jnp.sum(colsum * self_dots, axis=-1))
    trace_terms = jnp.sum(kernel, axis=(-2, -1)) * (2.0 * STATE) / band - 4.0 / (band * band) * jnp.sum(kernel * own_dist, axis=(-2, -1))
    return force, jnp.sum(cross_terms + trace_terms)


def reference(particles, bias, spread, precision, coupling_h, coupling_v):
    padded = jnp.pad(particles, ((1, 1), (1, 1), (0, 0), (0, 0)))

    def one_row(row_index):
        three_rows = lax.dynamic_slice_in_dim(padded, row_index, 3, 0)
        distance = distances(three_rows)
        own_dist = distance[1:2, 1:-1]
        blanket = own_dist + distance[0:1, 1:-1] + distance[2:3, 1:-1] + distance[1:2, :-2] + distance[1:2, 2:]
        centre = three_rows[1:2, 1:-1]
        bias_row = lax.dynamic_slice_in_dim(bias, row_index, 1, 0)
        band_row = lax.dynamic_slice_in_dim(spread, row_index, 1, 0)
        scores = (-mixing(precision, centre) + bias_row[..., None]
                  + mixing(coupling_h, three_rows[1:2, 2:]) + mixing_t(coupling_h, three_rows[1:2, :-2])
                  + mixing(coupling_v, three_rows[2:3, 1:-1]) + mixing_t(coupling_v, three_rows[0:1, 1:-1]))
        force, partial_sum = finish(centre, scores, blanket, own_dist, band_row)
        return force[0], partial_sum

    forces, partial_sums = lax.map(one_row, jnp.arange(NROWS, dtype=jnp.int32))
    stein = jnp.sum(partial_sums) / (NROWS * NCOLS * PARTICLES * PARTICLES)
    return forces, stein
```

```python
import functools
import math

import jax
import jax.numpy as jnp
from jax import lax
from jax.experimental import pallas as pl
from jax.experimental.pallas import tpu as pltpu
from jax.sharding import PartitionSpec as P

MESH = pl.DeviceIdType.MESH
F32 = jnp.float32
BF16 = jnp.bfloat16
LOG2E = math.log2(math.e)


def row_fold(values):
    parts = [values[8 * i : 8 * i + 8] for i in range(values.shape[0] // 8)]
    while len(parts) > 1:
        parts = [a + b for a, b in zip(parts[::2], parts[1::2])]
    return parts[0]


def replicated_sum(values):
    folded = row_fold(values)
    return jnp.broadcast_to(jnp.sum(folded, axis=0, keepdims=True), folded.shape)


def top_bits(values):
    scaled = values * 65537.0
    return scaled - (scaled - values)


def split3(values):
    first = top_bits(values)
    rest = values - first
    second = top_bits(rest)
    return first, second, rest - second


class Kernel:
    def __init__(self, n_gx, n_gy, rows, cols):
        self.n_gx, self.n_gy, self.rows, self.cols = n_gx, n_gy, rows, cols
        self.brows, self.bcols = rows // 2, cols // 2

    def block_of(self, k):
        br, bc = self.brows, self.bcols
        inner = (br - 2) * (bc - 2)
        k1 = k - inner
        k2 = k1 - 2 * (bc - 2)
        k3 = k2 - 2 * (br - 2)
        where = lambda cond, a, b: lax.select(cond, jnp.int32(a), jnp.int32(b))
        k = jnp.int32(k)
        kk = jnp.maximum(jnp.int32(k), 0)
        k1 = jnp.maximum(jnp.int32(k1), 0)
        k2 = jnp.maximum(jnp.int32(k2), 0)
        k3 = jnp.maximum(jnp.int32(k3), 0)
        bi = where(k < inner, 1 + kk // (bc - 2), 0)
        bj = where(k < inner, 1 + kk % (bc - 2), 0)
        on1 = (k >= inner) & (k < inner + 2 * (bc - 2))
        bi = where(on1, (br - 1) * (k1 % 2), bi)
        bj = where(on1, 1 + k1 // 2, bj)
        on2 = (k >= inner + 2 * (bc - 2)) & (k < inner + 2 * (bc - 2) + 2 * (br - 2))
        bi = where(on2, 1 + k2 // 2, bi)
        bj = where(on2, (bc - 1) * (k2 % 2), bj)
        on3 = k >= inner + 2 * (bc - 2) + 2 * (br - 2)
        bi = where(on3, (br - 1) * (k3 // 2), bi)
        bj = where(on3, (bc - 1) * (k3 % 2), bj)
        return bi, bj

    def __call__(
        self, x_hbm, bias_ref, spread_ref, prec_ref, ch_ref, cv_ref, out_hbm, stein_ref,
        xp, sq, fo, klow0, klow1, st0, st1, cs0, cs1, qs0, qs1, wq, wv, whb, acc, ar_stage, ar1, ar2,
        load_sem, out_sem, hs_send, hs_recv, vs_send, vs_recv, a1_send, a1_recv, a2_send, a2_recv,
    ):
        rows, cols, n_gx, n_gy = self.rows, self.cols, self.n_gx, self.n_gy
        brows, bcols = self.brows, self.bcols
        gx, gy = lax.axis_index("gx"), lax.axis_index("gy")

        loads = [
            pltpu.make_async_copy(
                x_hbm.at[pl.ds(2 * i, 2)], xp.at[pl.ds(1 + 2 * i, 2), pl.ds(1, cols)], load_sem.at[i]
            )
            for i in range(brows)
        ]
        for copy in loads:
            copy.start()
        barrier = pltpu.get_barrier_semaphore()
        for off in range(1, n_gx):
            pl.semaphore_signal(
                barrier, inc=1, device_id={"gx": lax.rem(gx + off, n_gx), "gy": gy}, device_id_type=MESH
            )
        for off in range(1, n_gy):
            pl.semaphore_signal(
                barrier, inc=1, device_id={"gx": gx, "gy": lax.rem(gy + off, n_gy)}, device_id_type=MESH
            )

        minus_a = (-(prec_ref[...].astype(F32))).astype(BF16)
        h_mat, v_mat = ch_ref[...], cv_ref[...]
        h_t, v_t = h_mat.T, v_mat.T
        zero = jnp.zeros_like(h_mat)
        table = [
            [minus_a, h_mat, v_mat, zero],
            [h_t, minus_a, zero, v_mat],
            [v_t, zero, minus_a, h_mat],
            [zero, v_t, h_t, minus_a],
        ]
        for a in range(4):
            wq[64 * a : 64 * a + 64, :] = jnp.concatenate(table[a], axis=1)
        wv[0] = jnp.concatenate([zero, v_t], axis=1)
        wv[1] = jnp.concatenate([zero, v_mat], axis=1)
        for r in range(rows):
            parts = [p.astype(BF16) for p in split3(bias_ref[r])]
            tail = jnp.concatenate([jnp.zeros((16, 64), BF16)] + parts, axis=0)
            tail_t = tail.T
            whb[r, 0] = jnp.concatenate([h_t, tail_t], axis=1)
            whb[r, 1] = jnp.concatenate([h_mat, tail_t], axis=1)
        acc[...] = jnp.zeros_like(acc)

        def clear(row, row_count, col, col_count):
            def one(t, _):
                r, c = row + t // col_count, col + t % col_count
                xp[r, c] = jnp.zeros((64, 256), BF16)
                sq[r, c] = jnp.zeros((8, 256), F32)
                return 0

            lax.fori_loop(0, row_count * col_count, one, 0)

        has_up, has_down = gx > 0, gx < n_gx - 1
        has_left, has_right = gy > 0, gy < n_gy - 1
        pl.when(jnp.logical_not(has_up))(lambda: clear(0, 1, 1, cols))
        pl.when(jnp.logical_not(has_down))(lambda: clear(rows + 1, 1, 1, cols))
        pl.when(jnp.logical_not(has_left))(lambda: clear(1, rows, 0, 1))
        pl.when(jnp.logical_not(has_right))(lambda: clear(1, rows, cols + 1, 1))

        def down_copy(j):
            return pltpu.make_async_remote_copy(
                src_ref=x_hbm.at[pl.ds(rows - 1, 1), pl.ds(2 * j, 2)],
                dst_ref=xp.at[pl.ds(0, 1), pl.ds(1 + 2 * j, 2)],
                send_sem=vs_send.at[0, j], recv_sem=vs_recv.at[0, j],
                device_id={"gx": lax.rem(gx + 1, n_gx), "gy": gy}, device_id_type=MESH,
            )

        def up_copy(j):
            return pltpu.make_async_remote_copy(
                src_ref=x_hbm.at[pl.ds(0, 1), pl.ds(2 * j, 2)],
                dst_ref=xp.at[pl.ds(rows + 1, 1), pl.ds(1 + 2 * j, 2)],
                send_sem=vs_send.at[1, j], recv_sem=vs_recv.at[1, j],
                device_id={"gx": lax.rem(gx + n_gx - 1, n_gx), "gy": gy}, device_id_type=MESH,
            )

        def right_copy(i):
            return pltpu.make_async_remote_copy(
                src_ref=x_hbm.at[pl.ds(2 * i, 2), pl.ds(cols - 1, 1)],
                dst_ref=xp.at[pl.ds(1 + 2 * i, 2), pl.ds(0, 1)],
                send_sem=hs_send.at[0, i], recv_sem=hs_recv.at[0, i],
                device_id={"gx": gx, "gy": lax.rem(gy + 1, n_gy)}, device_id_type=MESH,
            )

        def left_copy(i):
            return pltpu.make_async_remote_copy(
                src_ref=x_hbm.at[pl.ds(2 * i, 2), pl.ds(0, 1)],
                dst_ref=xp.at[pl.ds(1 + 2 * i, 2), pl.ds(cols + 1, 1)],
                send_sem=hs_send.at[1, i], recv_sem=hs_recv.at[1, i],
                device_id={"gx": gx, "gy": lax.rem(gy + n_gy - 1, n_gy)}, device_id_type=MESH,
            )

        v_order = list(range(1, bcols - 1)) + [0, bcols - 1]
        h_order = list(range(1, brows - 1)) + [0, brows - 1]
        pl.semaphore_wait(barrier, n_gx + n_gy - 2)

        @pl.when(has_down)
        def _():
            for j in v_order:
                down_copy(j).start()

        @pl.when(has_up)
        def _():
            for j in v_order:
                up_copy(j).start()

        @pl.when(has_right)
        def _():
            for i in h_order:
                right_copy(i).start()

        @pl.when(has_left)
        def _():
            for i in h_order:
                left_copy(i).start()

        def norms(r, c):
            values = xp[r, c].astype(F32)
            sq[r, c] = replicated_sum(values * values)

        for i in range(brows):
            loads[i].wait()

            def norm_pair(t, _, i=i):
                norms(1 + 2 * i, 1 + t)
                norms(2 + 2 * i, 1 + t)
                return 0

            lax.fori_loop(0, cols, norm_pair, 0)

        def arrive(bi, bj):
            @pl.when((bi == 0) & has_up)
            def _():
                down_copy(bj).wait_recv()
                norms(0, 1 + 2 * bj)
                norms(0, 2 + 2 * bj)

            @pl.when((bi == brows - 1) & has_down)
            def _():
                up_copy(bj).wait_recv()
                norms(rows + 1, 1 + 2 * bj)
                norms(rows + 1, 2 + 2 * bj)

            @pl.when((bj == 0) & has_left)
            def _():
                right_copy(bi).wait_recv()
                norms(1 + 2 * bi, 0)
                norms(2 + 2 * bi, 0)

            @pl.when((bj == bcols - 1) & has_right)
            def _():
                left_copy(bi).wait_recv()
                norms(1 + 2 * bi, cols + 1)
                norms(2 + 2 * bi, cols + 1)

        row8 = lax.broadcasted_iota(jnp.int32, (8, 256), 0)
        hot_row = lax.broadcasted_iota(jnp.int32, (48, 256), 0)
        dims = (((1,), (0,)), ((), ()))
        dot = functools.partial(lax.dot_general, dimension_numbers=dims, preferred_element_type=F32)

        def stage_a(k, klow, st, cs, qs):
            bi, bj = self.block_of(k)
            r0, c0 = 1 + 2 * bi, 1 + 2 * bj
            at = lambda a, b: xp[r0 + a, c0 + b]
            own = [at(0, 0), at(0, 1), at(1, 0), at(1, 1)]
            q_rhs = jnp.concatenate(own, axis=0)
            q = dot(jnp.concatenate([q_rhs.T, wq[...]], axis=0), q_rhs)
            qs[...] = q
            for n in range(4):
                a, b = n // 2, n % 2
                va, hb = (-1, 2)[a], (-1, 2)[b]
                opposite, vert, horiz = own[3 - n], at(va, b), at(a, hb)
                total = (
                    (sq[r0 + a, c0 + b] + sq[r0 + va, c0 + b])
                    + (sq[r0 + a, c0 + hb] + sq[r0 + 1 - a, c0 + b])
                    + sq[r0 + a, c0 + 1 - b]
                )
                s1, s2, s3 = split3(total * -0.5)
                stack = lambda x0, x1: jnp.where(
                    row8 == x0, s1, jnp.where(row8 == x0 + 1, s2, jnp.where(row8 == x0 + 2, s3, jnp.where(
                        (row8 >= x1) & (row8 < x1 + 3), 1.0, 0.0)))
                )
                zeros8 = jnp.zeros((8, 256), F32)
                aug_r = jnp.concatenate([stack(3, 0), zeros8], axis=0).astype(BF16)
                aug_l = jnp.concatenate([stack(0, 3), zeros8], axis=0).astype(BF16)
                col = 2 * bj + b
                hot = jnp.where(
                    (hot_row == col) | (hot_row == col + 16) | (hot_row == col + 32), 1.0, 0.0
                ).astype(BF16)
                rhs = jnp.concatenate([opposite, vert, horiz, aug_r, hot], axis=0)
                lhs_t = jnp.concatenate([-opposite, vert, horiz, aug_l, jnp.zeros((48, 256), BF16)], axis=0)
                weight = jnp.concatenate([wv[a], whb[2 * bi + a, b]], axis=1)
                rest = dot(jnp.concatenate([lhs_t.T, weight], axis=0), rhs)
                h = spread_ref[2 * bi + a, 2 * bj + b]
                kernel = jnp.exp2((qs[0:256] + rest[0:256]) * (2.0 * LOG2E / h))
                klow[n] = kernel.astype(BF16)
                cs[n] = replicated_sum(kernel)
                score = qs[256 + 64 * n : 320 + 64 * n] + rest[256:320]
                st[n, 0:64] = score.astype(BF16)
                st[n, 64:128] = own[n]

        def stage_c(k, klow, st, cs):
            bi, bj = self.block_of(k)
            total = acc[...]
            for n in range(4):
                a, b = n // 2, n % 2
                h = spread_ref[2 * bi + a, 2 * bj + b]
                scale = 2.0 / h
                prod = dot(st[n], klow[n])
                pull, push = prod[0:64], prod[64:128]
                s = st[n, 0:64].astype(F32)
                x = st[n, 64:128].astype(F32)
                colsum = cs[n]
                v = (push - x * jnp.concatenate([colsum] * 8, axis=0)) * scale
                force = pull - v
                fo[2 * bi + a, 2 * bj + b] = force.astype(BF16)
                total = total + row_fold(s * (force - v)) + (2.0 * scale) * row_fold(x * v) + (8.0 * scale) * colsum
            acc[...] = total

        def out_copy(bi, bj):
            window = (pl.ds(2 * bi, 2), pl.ds(2 * bj, 2))
            return pltpu.make_async_copy(fo.at[window], out_hbm.at[window], out_sem.at[bi, bj])

        def ship(k):
            bi, bj = self.block_of(k)
            out_copy(bi, bj).start()

        blocks = brows * bcols
        set0, set1 = (klow0, st0, cs0), (klow1, st1, cs1)
        arrive(*self.block_of(0))
        stage_a(0, *set0, qs0)

        def body(j, _):
            arrive(*self.block_of(2 * j + 1))
            arrive(*self.block_of(2 * j + 2))
            stage_a(2 * j + 1, *set1, qs1)
            stage_c(2 * j, *set0)
            stage_a(2 * j + 2, *set0, qs0)
            stage_c(2 * j + 1, *set1)
            ship(2 * j)
            ship(2 * j + 1)
            return 0

        lax.fori_loop(0, blocks // 2 - 1, body, 0)
        arrive(*self.block_of(blocks - 1))
        stage_a(blocks - 1, *set1, qs1)
        stage_c(blocks - 2, *set0)
        stage_c(blocks - 1, *set1)
        ship(blocks - 2)
        ship(blocks - 1)

        ar_stage[0] = acc[:, 0:128] + acc[:, 128:256]
        ar1[gx] = ar_stage[0]

        def a1_copy(off):
            return pltpu.make_async_remote_copy(
                src_ref=ar_stage.at[0], dst_ref=ar1.at[gx],
                send_sem=a1_send.at[off - 1], recv_sem=a1_recv.at[off - 1],
                device_id={"gx": lax.rem(gx + off, n_gx), "gy": gy}, device_id_type=MESH,
            )

        def a2_copy(off):
            return pltpu.make_async_remote_copy(
                src_ref=ar_stage.at[1], dst_ref=ar2.at[gy],
                send_sem=a2_send.at[off - 1], recv_sem=a2_recv.at[off - 1],
                device_id={"gx": gx, "gy": lax.rem(gy + off, n_gy)}, device_id_type=MESH,
            )

        for off in range(1, n_gx):
            a1_copy(off).start()
        for off in range(1, n_gx):
            a1_copy(off).wait_recv()
        total = ar1[0]
        for i in range(1, n_gx):
            total = total + ar1[i]
        ar_stage[1] = total
        ar2[gy] = total
        for off in range(1, n_gy):
            a2_copy(off).start()
        for off in range(1, n_gy):
            a2_copy(off).wait_recv()
        total = ar2[0]
        for i in range(1, n_gy):
            total = total + ar2[i]
        pairs = float(rows * n_gx * cols * n_gy * 256 * 256)
        stein_ref[0, 0] = jnp.sum(total) / pairs

        for off in range(1, n_gx):
            a1_copy(off).wait_send()
        for off in range(1, n_gy):
            a2_copy(off).wait_send()

        @pl.when(has_down)
        def _():
            for j in v_order:
                down_copy(j).wait_send()

        @pl.when(has_up)
        def _():
            for j in v_order:
                up_copy(j).wait_send()

        @pl.when(has_right)
        def _():
            for i in h_order:
                right_copy(i).wait_send()

        @pl.when(has_left)
        def _():
            for i in h_order:
                left_copy(i).wait_send()

        for bi in range(brows):
            for bj in range(bcols):
                out_copy(bi, bj).wait()


def solution(mesh):
    n_gx, n_gy = mesh.shape["gx"], mesh.shape["gy"]

    def step(particles, bias, spread, precision, coupling_h, coupling_v):
        rows, cols = particles.shape[:2]
        dma = pltpu.SemaphoreType.DMA
        vmem = pl.BlockSpec(memory_space=pltpu.VMEM)
        hbm = pl.BlockSpec(memory_space=pl.ANY)
        smem = pl.BlockSpec(memory_space=pltpu.SMEM)
        force, stein = pl.pallas_call(
            Kernel(n_gx, n_gy, rows, cols),
            name="svgd",
            out_shape=(
                jax.ShapeDtypeStruct(particles.shape, BF16),
                jax.ShapeDtypeStruct((1, 1), F32),
            ),
            in_specs=[hbm, vmem, smem, vmem, vmem, vmem],
            out_specs=(hbm, smem),
            scratch_shapes=[
                pltpu.VMEM((rows + 2, cols + 2, 64, 256), BF16),
                pltpu.VMEM((rows + 2, cols + 2, 8, 256), F32),
                pltpu.VMEM((rows, cols, 64, 256), BF16),
                pltpu.VMEM((4, 256, 256), BF16),
                pltpu.VMEM((4, 256, 256), BF16),
                pltpu.VMEM((4, 128, 256), BF16),
                pltpu.VMEM((4, 128, 256), BF16),
                pltpu.VMEM((4, 8, 256), F32),
                pltpu.VMEM((4, 8, 256), F32),
                pltpu.VMEM((512, 256), F32),
                pltpu.VMEM((512, 256), F32),
                pltpu.VMEM((256, 256), BF16),
                pltpu.VMEM((2, 64, 128), BF16),
                pltpu.VMEM((rows, 2, 64, 128), BF16),
                pltpu.VMEM((8, 256), F32),
                pltpu.VMEM((2, 8, 128), F32),
                pltpu.VMEM((n_gx, 8, 128), F32),
                pltpu.VMEM((n_gy, 8, 128), F32),
                dma((rows // 2,)),
                dma((rows // 2, cols // 2)),
                dma((2, rows // 2)),
                dma((2, rows // 2)),
                dma((2, cols // 2)),
                dma((2, cols // 2)),
                dma((n_gx - 1,)),
                dma((n_gx - 1,)),
                dma((n_gy - 1,)),
                dma((n_gy - 1,)),
            ],
            compiler_params=pltpu.CompilerParams(collective_id=0, has_side_effects=True, vmem_limit_bytes=48 * 2**20),
        )(particles, bias, spread, precision, coupling_h, coupling_v)
        return force, stein[0, 0]

    return jax.shard_map(
        step,
        mesh=mesh,
        in_specs=(P("gx", "gy", None, None), P("gx", "gy", None), P("gx", "gy"), P(), P(), P()),
        out_specs=(P("gx", "gy", None, None), P()),
        check_vma=False,
    )
```

```python
import functools
import math

import jax
import jax.numpy as jnp
from jax import lax
from jax.experimental import pallas as pl
from jax.experimental.pallas import tpu as pltpu
from jax.sharding import PartitionSpec as P

MESH = pl.DeviceIdType.MESH
F32 = jnp.float32
BF16 = jnp.bfloat16
LOG2E = math.log2(math.e)


def row_fold(values):
    parts = [values[8 * i : 8 * i + 8] for i in range(values.shape[0] // 8)]
    while len(parts) > 1:
        parts = [a + b for a, b in zip(parts[::2], parts[1::2])]
    return parts[0]


def replicated_sum(values):
    folded = row_fold(values)
    return jnp.broadcast_to(jnp.sum(folded, axis=0, keepdims=True), folded.shape)


def top_bits(values):
    scaled = values * 65537.0
    return scaled - (scaled - values)


def split3(values):
    first = top_bits(values)
    rest = values - first
    second = top_bits(rest)
    return first, second, rest - second


class Kernel:
    def __init__(self, n_gx, n_gy, rows, cols):
        self.n_gx, self.n_gy, self.rows, self.cols = n_gx, n_gy, rows, cols
        self.brows, self.bcols = rows // 2, cols // 2

    def block_of(self, k):
        br, bc = self.brows, self.bcols
        inner = (br - 2) * (bc - 2)
        k1 = k - inner
        k2 = k1 - 2 * (bc - 2)
        k3 = k2 - 2 * (br - 2)
        where = lambda cond, a, b: lax.select(cond, jnp.int32(a), jnp.int32(b))
        k = jnp.int32(k)
        kk = jnp.maximum(jnp.int32(k), 0)
        k1 = jnp.maximum(jnp.int32(k1), 0)
        k2 = jnp.maximum(jnp.int32(k2), 0)
        k3 = jnp.maximum(jnp.int32(k3), 0)
        bi = where(k < inner, 1 + kk // (bc - 2), 0)
        bj = where(k < inner, 1 + kk % (bc - 2), 0)
        on1 = (k >= inner) & (k < inner + 2 * (bc - 2))
        bi = where(on1, (br - 1) * (k1 % 2), bi)
        bj = where(on1, 1 + k1 // 2, bj)
        on2 = (k >= inner + 2 * (bc - 2)) & (k < inner + 2 * (bc - 2) + 2 * (br - 2))
        bi = where(on2, 1 + k2 // 2, bi)
        bj = where(on2, (bc - 1) * (k2 % 2), bj)
        on3 = k >= inner + 2 * (bc - 2) + 2 * (br - 2)
        bi = where(on3, (br - 1) * (k3 // 2), bi)
        bj = where(on3, (bc - 1) * (k3 % 2), bj)
        return bi, bj

    def __call__(
        self, x_hbm, bias_hbm, spread_hbm, prec_hbm, ch_hbm, cv_hbm, out_hbm, stein_ref,
        bias_ref, spread_ref, prec_ref, ch_ref, cv_ref, small_sem, xp, sq, fo, klow, st, qs, hot, base_l, base_r, wq, wv, whb, acc, ar_stage, ar1, ar2,
        load_sem, out_sem, hs_send, hs_recv, vs_send, vs_recv, a1_send, a1_recv, a2_send, a2_recv,
    ):
        rows, cols, n_gx, n_gy = self.rows, self.cols, self.n_gx, self.n_gy
        brows, bcols = self.brows, self.bcols
        gx, gy = lax.axis_index("gx"), lax.axis_index("gy")

        loads = [
            pltpu.make_async_copy(
                x_hbm.at[pl.ds(2 * i, 2)], xp.at[pl.ds(1 + 2 * i, 2), pl.ds(1, cols)], load_sem.at[i]
            )
            for i in range(brows)
        ]
        smalls = [
            pltpu.make_async_copy(src, dst, small_sem.at[i])
            for i, (src, dst) in enumerate(
                [(prec_hbm, prec_ref), (ch_hbm, ch_ref), (cv_hbm, cv_ref), (bias_hbm, bias_ref), (spread_hbm, spread_ref)]
            )
        ]
        for copy in smalls + loads:
            copy.start()
        barrier = pltpu.get_barrier_semaphore()
        for off in range(1, n_gx):
            pl.semaphore_signal(
                barrier, inc=1, device_id={"gx": lax.rem(gx + off, n_gx), "gy": gy}, device_id_type=MESH
            )
        for off in range(1, n_gy):
            pl.semaphore_signal(
                barrier, inc=1, device_id={"gx": gx, "gy": lax.rem(gy + off, n_gy)}, device_id_type=MESH
            )

        for copy in smalls:
            copy.wait()
        minus_a = (-(prec_ref[...].astype(F32))).astype(BF16)
        h_mat, v_mat = ch_ref[...], cv_ref[...]
        h_t, v_t = h_mat.T, v_mat.T
        zero = jnp.zeros_like(h_mat)
        table = [
            [minus_a, h_mat, v_mat, zero],
            [h_t, minus_a, zero, v_mat],
            [v_t, zero, minus_a, h_mat],
            [zero, v_t, h_t, minus_a],
        ]
        for a in range(4):
            wq[64 * a : 64 * a + 64, :] = jnp.concatenate(table[a], axis=1)
        wv[0] = jnp.concatenate([zero, v_t], axis=1)
        wv[1] = jnp.concatenate([zero, v_mat], axis=1)
        for r in range(rows):
            parts = [p.astype(BF16) for p in split3(bias_ref[r])]
            tail = jnp.concatenate([jnp.zeros((16, 64), BF16)] + parts, axis=0)
            tail_t = tail.T
            whb[r, 0] = jnp.concatenate([h_t, tail_t], axis=1)
            whb[r, 1] = jnp.concatenate([h_mat, tail_t], axis=1)
        acc[...] = jnp.zeros_like(acc)
        row = lax.broadcasted_iota(jnp.int32, (8, 256), 0)
        for slot in range(2):
            for n in range(4):
                st[slot, n, 128:144] = jnp.ones((16, 256), BF16)
        base_r[...] = jnp.where(row < 3, 1.0, 0.0)
        base_l[...] = jnp.where((row >= 3) & (row < 6), 1.0, 0.0)
        hot_row = lax.broadcasted_iota(jnp.int32, (48, 256), 0) % 16

        def one_hot(col, _):
            hot[col] = jnp.where(hot_row == col, 1.0, 0.0).astype(BF16)
            return 0

        lax.fori_loop(0, cols, one_hot, 0)

        def clear(row, row_count, col, col_count):
            def one(t, _):
                r, c = row + t // col_count, col + t % col_count
                xp[r, c] = jnp.zeros((64, 256), BF16)
                sq[r, c] = jnp.zeros((8, 256), F32)
                return 0

            lax.fori_loop(0, row_count * col_count, one, 0)

        has_up, has_down = gx > 0, gx < n_gx - 1
        has_left, has_right = gy > 0, gy < n_gy - 1
        pl.when(jnp.logical_not(has_up))(lambda: clear(0, 1, 1, cols))
        pl.when(jnp.logical_not(has_down))(lambda: clear(rows + 1, 1, 1, cols))
        pl.when(jnp.logical_not(has_left))(lambda: clear(1, rows, 0, 1))
        pl.when(jnp.logical_not(has_right))(lambda: clear(1, rows, cols + 1, 1))

        def down_copy(j):
            return pltpu.make_async_remote_copy(
                src_ref=x_hbm.at[pl.ds(rows - 1, 1), pl.ds(2 * j, 2)],
                dst_ref=xp.at[pl.ds(0, 1), pl.ds(1 + 2 * j, 2)],
                send_sem=vs_send.at[0, j], recv_sem=vs_recv.at[0, j],
                device_id={"gx": lax.rem(gx + 1, n_gx), "gy": gy}, device_id_type=MESH,
            )

        def up_copy(j):
            return pltpu.make_async_remote_copy(
                src_ref=x_hbm.at[pl.ds(0, 1), pl.ds(2 * j, 2)],
                dst_ref=xp.at[pl.ds(rows + 1, 1), pl.ds(1 + 2 * j, 2)],
                send_sem=vs_send.at[1, j], recv_sem=vs_recv.at[1, j],
                device_id={"gx": lax.rem(gx + n_gx - 1, n_gx), "gy": gy}, device_id_type=MESH,
            )

        def right_copy(i):
            return pltpu.make_async_remote_copy(
                src_ref=x_hbm.at[pl.ds(2 * i, 2), pl.ds(cols - 1, 1)],
                dst_ref=xp.at[pl.ds(1 + 2 * i, 2), pl.ds(0, 1)],
                send_sem=hs_send.at[0, i], recv_sem=hs_recv.at[0, i],
                device_id={"gx": gx, "gy": lax.rem(gy + 1, n_gy)}, device_id_type=MESH,
            )

        def left_copy(i):
            return pltpu.make_async_remote_copy(
                src_ref=x_hbm.at[pl.ds(2 * i, 2), pl.ds(0, 1)],
                dst_ref=xp.at[pl.ds(1 + 2 * i, 2), pl.ds(cols + 1, 1)],
                send_sem=hs_send.at[1, i], recv_sem=hs_recv.at[1, i],
                device_id={"gx": gx, "gy": lax.rem(gy + n_gy - 1, n_gy)}, device_id_type=MESH,
            )

        v_order = list(range(1, bcols - 1)) + [0, bcols - 1]
        h_order = list(range(1, brows - 1)) + [0, brows - 1]
        pl.semaphore_wait(barrier, n_gx + n_gy - 2)

        @pl.when(has_down)
        def _():
            for j in v_order:
                down_copy(j).start()

        @pl.when(has_up)
        def _():
            for j in v_order:
                up_copy(j).start()

        @pl.when(has_right)
        def _():
            for i in h_order:
                right_copy(i).start()

        @pl.when(has_left)
        def _():
            for i in h_order:
                left_copy(i).start()

        def norms(r, c):
            values = xp[r, c].astype(F32)
            sq[r, c] = replicated_sum(values * values)

        for i in range(brows):
            loads[i].wait()

            def norm_pair(t, _, i=i):
                norms(1 + 2 * i, 1 + t)
                norms(2 + 2 * i, 1 + t)
                return 0

            lax.fori_loop(0, cols, norm_pair, 0)

        def arrive(bi, bj):
            @pl.when((bi == 0) & has_up)
            def _():
                down_copy(bj).wait_recv()
                norms(0, 1 + 2 * bj)
                norms(0, 2 + 2 * bj)

            @pl.when((bi == brows - 1) & has_down)
            def _():
                up_copy(bj).wait_recv()
                norms(rows + 1, 1 + 2 * bj)
                norms(rows + 1, 2 + 2 * bj)

            @pl.when((bj == 0) & has_left)
            def _():
                right_copy(bi).wait_recv()
                norms(1 + 2 * bi, 0)
                norms(2 + 2 * bi, 0)

            @pl.when((bj == bcols - 1) & has_right)
            def _():
                left_copy(bi).wait_recv()
                norms(1 + 2 * bi, cols + 1)
                norms(2 + 2 * bi, cols + 1)

        row8 = lax.broadcasted_iota(jnp.int32, (8, 256), 0)
        dims = (((1,), (0,)), ((), ()))
        dot = functools.partial(lax.dot_general, dimension_numbers=dims, preferred_element_type=F32)

        def stage_a(k, slot):
            bi, bj = self.block_of(k)
            r0, c0 = 1 + 2 * bi, 1 + 2 * bj
            at = lambda a, b: xp[r0 + a, c0 + b]
            own = [at(0, 0), at(0, 1), at(1, 0), at(1, 1)]
            q_rhs = jnp.concatenate(own, axis=0)
            qs[slot] = dot(jnp.concatenate([q_rhs.T, wq[...]], axis=0), q_rhs)
            for n in range(4):
                a, b = n // 2, n % 2
                va, hb = (-1, 2)[a], (-1, 2)[b]
                opposite, vert, horiz = own[3 - n], at(va, b), at(a, hb)
                total = (
                    (sq[r0 + a, c0 + b] + sq[r0 + va, c0 + b])
                    + (sq[r0 + a, c0 + hb] + sq[r0 + 1 - a, c0 + b])
                    + sq[r0 + a, c0 + 1 - b]
                )
                s1, s2, s3 = split3(total * -0.5)
                pick = lambda base, x: jnp.where(
                    row8 == x, s1, jnp.where(row8 == x + 1, s2, jnp.where(row8 == x + 2, s3, base[...]))
                )
                zeros8 = jnp.zeros((8, 256), F32)
                aug_r = jnp.concatenate([pick(base_r, 3), zeros8], axis=0).astype(BF16)
                aug_l = jnp.concatenate([pick(base_l, 0), zeros8], axis=0).astype(BF16)
                rhs = jnp.concatenate([opposite, vert, horiz, aug_r, hot[2 * bj + b]], axis=0)
                lhs_t = jnp.concatenate([-opposite, vert, horiz, aug_l, jnp.zeros((48, 256), BF16)], axis=0)
                weight = jnp.concatenate([wv[a], whb[2 * bi + a, b]], axis=1)
                rest = dot(jnp.concatenate([lhs_t.T, weight], axis=0), rhs)
                h = spread_ref[2 * bi + a, 2 * bj + b]
                kernel = jnp.exp2((qs[slot, 0:256] + rest[0:256]) * (2.0 * LOG2E / h))
                klow[slot, n] = kernel.astype(BF16)
                score = qs[slot, 256 + 64 * n : 320 + 64 * n] + rest[256:320]
                st[slot, n, 0:64] = score.astype(BF16)
                st[slot, n, 64:128] = own[n]

        def stage_c(k, slot):
            bi, bj = self.block_of(k)
            total = acc[...]
            for n in range(4):
                a, b = n // 2, n % 2
                h = spread_ref[2 * bi + a, 2 * bj + b]
                scale = 2.0 / h
                prod = dot(st[slot, n], klow[slot, n])
                pull, push, colsum = prod[0:64], prod[64:128], prod[128:136]
                s = st[slot, n, 0:64].astype(F32)
                x = st[slot, n, 64:128].astype(F32)
                v = (push - x * jnp.concatenate([colsum] * 8, axis=0)) * scale
                force = pull - v
                fo[2 * bi + a, 2 * bj + b] = force.astype(BF16)
                total = total + row_fold(s * (force - v)) + (2.0 * scale) * row_fold(x * v) + (8.0 * scale) * colsum
            acc[...] = total

        def out_copy(bi, bj):
            window = (pl.ds(2 * bi, 2), pl.ds(2 * bj, 2))
            return pltpu.make_async_copy(fo.at[window], out_hbm.at[window], out_sem.at[bi, bj])

        def ship(k):
            bi, bj = self.block_of(k)
            out_copy(bi, bj).start()

        blocks = brows * bcols

        def pair_arrives(j):
            @pl.when(2 * j + 1 >= (brows - 2) * (bcols - 2))
            def _():
                arrive(*self.block_of(2 * j))
                arrive(*self.block_of(2 * j + 1))

        stage_a(0, 0)
        stage_a(1, 1)

        def body(j, _):
            pair_arrives(j + 1)
            stage_c(2 * j, 0)
            stage_c(2 * j + 1, 1)
            stage_a(2 * j + 2, 0)
            stage_a(2 * j + 3, 1)
            ship(2 * j)
            ship(2 * j + 1)
            return 0

        lax.fori_loop(0, blocks // 2 - 1, body, 0)
        stage_c(blocks - 2, 0)
        stage_c(blocks - 1, 1)
        ship(blocks - 2)
        ship(blocks - 1)

        ar_stage[0] = acc[:, 0:128] + acc[:, 128:256]
        ar1[gx] = ar_stage[0]

        def a1_copy(off):
            return pltpu.make_async_remote_copy(
                src_ref=ar_stage.at[0], dst_ref=ar1.at[gx],
                send_sem=a1_send.at[off - 1], recv_sem=a1_recv.at[off - 1],
                device_id={"gx": lax.rem(gx + off, n_gx), "gy": gy}, device_id_type=MESH,
            )

        def a2_copy(off):
            return pltpu.make_async_remote_copy(
                src_ref=ar_stage.at[1], dst_ref=ar2.at[gy],
                send_sem=a2_send.at[off - 1], recv_sem=a2_recv.at[off - 1],
                device_id={"gx": gx, "gy": lax.rem(gy + off, n_gy)}, device_id_type=MESH,
            )

        for off in range(1, n_gx):
            a1_copy(off).start()
        for off in range(1, n_gx):
            a1_copy(off).wait_recv()
        total = ar1[0]
        for i in range(1, n_gx):
            total = total + ar1[i]
        ar_stage[1] = total
        ar2[gy] = total
        for off in range(1, n_gy):
            a2_copy(off).start()
        for off in range(1, n_gy):
            a2_copy(off).wait_recv()
        total = ar2[0]
        for i in range(1, n_gy):
            total = total + ar2[i]
        pairs = float(rows * n_gx * cols * n_gy * 256 * 256)
        stein_ref[0, 0] = jnp.sum(total) / pairs

        for off in range(1, n_gx):
            a1_copy(off).wait_send()
        for off in range(1, n_gy):
            a2_copy(off).wait_send()

        @pl.when(has_down)
        def _():
            for j in v_order:
                down_copy(j).wait_send()

        @pl.when(has_up)
        def _():
            for j in v_order:
                up_copy(j).wait_send()

        @pl.when(has_right)
        def _():
            for i in h_order:
                right_copy(i).wait_send()

        @pl.when(has_left)
        def _():
            for i in h_order:
                left_copy(i).wait_send()

        for bi in range(brows):
            for bj in range(bcols):
                out_copy(bi, bj).wait()


def solution(mesh):
    n_gx, n_gy = mesh.shape["gx"], mesh.shape["gy"]

    def step(particles, bias, spread, precision, coupling_h, coupling_v):
        rows, cols = particles.shape[:2]
        dma = pltpu.SemaphoreType.DMA
        hbm = pl.BlockSpec(memory_space=pltpu.HBM)
        smem = pl.BlockSpec(memory_space=pltpu.SMEM)
        force, stein = pl.pallas_call(
            Kernel(n_gx, n_gy, rows, cols),
            name="svgd",
            out_shape=(
                jax.ShapeDtypeStruct(particles.shape, BF16),
                jax.ShapeDtypeStruct((1, 1), F32),
            ),
            in_specs=[hbm] * 6,
            out_specs=(hbm, smem),
            scratch_shapes=[
                pltpu.VMEM(bias.shape, F32),
                pltpu.SMEM(spread.shape, F32),
                pltpu.VMEM((64, 64), BF16),
                pltpu.VMEM((64, 64), BF16),
                pltpu.VMEM((64, 64), BF16),
                dma((5,)),
                pltpu.VMEM((rows + 2, cols + 2, 64, 256), BF16),
                pltpu.VMEM((rows + 2, cols + 2, 8, 256), F32),
                pltpu.VMEM((rows, cols, 64, 256), BF16),
                pltpu.VMEM((2, 4, 256, 256), BF16),
                pltpu.VMEM((2, 4, 144, 256), BF16),
                pltpu.VMEM((2, 512, 256), F32),
                pltpu.VMEM((cols, 48, 256), BF16),
                pltpu.VMEM((8, 256), F32),
                pltpu.VMEM((8, 256), F32),
                pltpu.VMEM((256, 256), BF16),
                pltpu.VMEM((2, 64, 128), BF16),
                pltpu.VMEM((rows, 2, 64, 128), BF16),
                pltpu.VMEM((8, 256), F32),
                pltpu.VMEM((2, 8, 128), F32),
                pltpu.VMEM((n_gx, 8, 128), F32),
                pltpu.VMEM((n_gy, 8, 128), F32),
                dma((rows // 2,)),
                dma((rows // 2, cols // 2)),
                dma((2, rows // 2)),
                dma((2, rows // 2)),
                dma((2, cols // 2)),
                dma((2, cols // 2)),
                dma((n_gx - 1,)),
                dma((n_gx - 1,)),
                dma((n_gy - 1,)),
                dma((n_gy - 1,)),
            ],
            compiler_params=pltpu.CompilerParams(collective_id=0, has_side_effects=True, vmem_limit_bytes=50_000_000),
        )(particles, *(pltpu.with_memory_space_constraint(v, pltpu.HBM) for v in (bias, spread, precision, coupling_h, coupling_v)))
        return force, stein[0, 0]

    return jax.shard_map(
        step,
        mesh=mesh,
        in_specs=(P("gx", "gy", None, None), P("gx", "gy", None), P("gx", "gy"), P(), P(), P()),
        out_specs=(P("gx", "gy", None, None), P()),
        check_vma=False,
    )
```

```python
import functools
import math

import jax
import jax.numpy as jnp
from jax import lax
from jax.experimental import pallas as pl
from jax.experimental.pallas import tpu as pltpu
from jax.sharding import PartitionSpec as P

MESH = pl.DeviceIdType.MESH
F32 = jnp.float32
BF16 = jnp.bfloat16
LOG2E = math.log2(math.e)


def row_fold(values):
    parts = [values[8 * i : 8 * i + 8] for i in range(values.shape[0] // 8)]
    while len(parts) > 1:
        parts = [a + b for a, b in zip(parts[::2], parts[1::2])]
    return parts[0]


def replicated_sum(values):
    folded = row_fold(values)
    return jnp.broadcast_to(jnp.sum(folded, axis=0, keepdims=True), folded.shape)


def top_bits(values):
    scaled = values * 65537.0
    return scaled - (scaled - values)


def split3(values):
    first = top_bits(values)
    rest = values - first
    second = top_bits(rest)
    return first, second, rest - second


class Kernel:
    def __init__(self, n_gx, n_gy, rows, cols):
        self.n_gx, self.n_gy, self.rows, self.cols = n_gx, n_gy, rows, cols
        self.brows, self.bcols = rows // 2, cols // 2

    def block_of(self, k):
        br, bc = self.brows, self.bcols
        inner = (br - 2) * (bc - 2)
        k1 = k - inner
        k2 = k1 - 2 * (bc - 2)
        k3 = k2 - 2 * (br - 2)
        where = lambda cond, a, b: lax.select(cond, jnp.int32(a), jnp.int32(b))
        k = jnp.int32(k)
        kk = jnp.maximum(jnp.int32(k), 0)
        k1 = jnp.maximum(jnp.int32(k1), 0)
        k2 = jnp.maximum(jnp.int32(k2), 0)
        k3 = jnp.maximum(jnp.int32(k3), 0)
        bi = where(k < inner, 1 + kk // (bc - 2), 0)
        bj = where(k < inner, 1 + kk % (bc - 2), 0)
        on1 = (k >= inner) & (k < inner + 2 * (bc - 2))
        bi = where(on1, (br - 1) * (k1 % 2), bi)
        bj = where(on1, 1 + k1 // 2, bj)
        on2 = (k >= inner + 2 * (bc - 2)) & (k < inner + 2 * (bc - 2) + 2 * (br - 2))
        bi = where(on2, 1 + k2 // 2, bi)
        bj = where(on2, (bc - 1) * (k2 % 2), bj)
        on3 = k >= inner + 2 * (bc - 2) + 2 * (br - 2)
        bi = where(on3, (br - 1) * (k3 // 2), bi)
        bj = where(on3, (bc - 1) * (k3 % 2), bj)
        return bi, bj

    def __call__(
        self, x_hbm, bias_hbm, spread_hbm, prec_hbm, ch_hbm, cv_hbm, fo, stein_ref,
        bias_ref, spread_ref, prec_ref, ch_ref, cv_ref, small_sem, xp, sq, klow, st, qs, hot, base_l, base_r, wq, wv, whb, acc, ar_stage, ar_all,
        load_sem, hs_send, hs_recv, vs_send, vs_recv, ar_send, ar_recv, ready,
    ):
        rows, cols, n_gx, n_gy = self.rows, self.cols, self.n_gx, self.n_gy
        brows, bcols = self.brows, self.bcols
        gx, gy = lax.axis_index("gx"), lax.axis_index("gy")

        loads = [
            pltpu.make_async_copy(
                x_hbm.at[pl.ds(2 * i, 2)], xp.at[pl.ds(1 + 2 * i, 2), pl.ds(1, cols)], load_sem.at[i]
            )
            for i in range(brows)
        ]
        smalls = [
            pltpu.make_async_copy(src, dst, small_sem.at[i])
            for i, (src, dst) in enumerate(
                [(prec_hbm, prec_ref), (ch_hbm, ch_ref), (cv_hbm, cv_ref), (bias_hbm, bias_ref), (spread_hbm, spread_ref)]
            )
        ]
        for copy in smalls + loads:
            copy.start()
        barrier = pltpu.get_barrier_semaphore()
        for off in range(1, n_gx):
            pl.semaphore_signal(
                barrier, inc=1, device_id={"gx": lax.rem(gx + off, n_gx), "gy": gy}, device_id_type=MESH
            )
        for off in range(1, n_gy):
            pl.semaphore_signal(
                barrier, inc=1, device_id={"gx": gx, "gy": lax.rem(gy + off, n_gy)}, device_id_type=MESH
            )

        for copy in smalls:
            copy.wait()
        minus_a = (-(prec_ref[...].astype(F32))).astype(BF16)
        h_mat, v_mat = ch_ref[...], cv_ref[...]
        h_t, v_t = h_mat.T, v_mat.T
        zero = jnp.zeros_like(h_mat)
        table = [
            [minus_a, h_mat, v_mat, zero],
            [h_t, minus_a, zero, v_mat],
            [v_t, zero, minus_a, h_mat],
            [zero, v_t, h_t, minus_a],
        ]
        for a in range(4):
            wq[64 * a : 64 * a + 64, :] = jnp.concatenate(table[a], axis=1)
        wv[0] = jnp.concatenate([zero, v_t], axis=1)
        wv[1] = jnp.concatenate([zero, v_mat], axis=1)
        for r in range(rows):
            parts = [p.astype(BF16) for p in split3(bias_ref[r])]
            tail = jnp.concatenate([jnp.zeros((16, 64), BF16)] + parts, axis=0)
            tail_t = tail.T
            whb[r, 0] = jnp.concatenate([h_t, tail_t], axis=1)
            whb[r, 1] = jnp.concatenate([h_mat, tail_t], axis=1)
        acc[...] = jnp.zeros_like(acc)
        row = lax.broadcasted_iota(jnp.int32, (8, 256), 0)
        for slot in range(2):
            for n in range(4):
                st[slot, n, 128:144] = jnp.ones((16, 256), BF16)
        base_r[...] = jnp.where(row < 3, 1.0, 0.0)
        base_l[...] = jnp.where((row >= 3) & (row < 6), 1.0, 0.0)
        hot_row = lax.broadcasted_iota(jnp.int32, (48, 256), 0) % 16

        def one_hot(col, _):
            hot[col] = jnp.where(hot_row == col, 1.0, 0.0).astype(BF16)
            return 0

        lax.fori_loop(0, cols, one_hot, 0)

        def clear(row, row_count, col, col_count):
            def one(t, _):
                r, c = row + t // col_count, col + t % col_count
                xp[r, c] = jnp.zeros((64, 256), BF16)
                sq[r, c] = jnp.zeros((8, 256), F32)
                return 0

            lax.fori_loop(0, row_count * col_count, one, 0)

        has_up, has_down = gx > 0, gx < n_gx - 1
        has_left, has_right = gy > 0, gy < n_gy - 1
        pl.when(jnp.logical_not(has_up))(lambda: clear(0, 1, 1, cols))
        pl.when(jnp.logical_not(has_down))(lambda: clear(rows + 1, 1, 1, cols))
        pl.when(jnp.logical_not(has_left))(lambda: clear(1, rows, 0, 1))
        pl.when(jnp.logical_not(has_right))(lambda: clear(1, rows, cols + 1, 1))

        def down_copy(j):
            return pltpu.make_async_remote_copy(
                src_ref=x_hbm.at[pl.ds(rows - 1, 1), pl.ds(2 * j, 2)],
                dst_ref=xp.at[pl.ds(0, 1), pl.ds(1 + 2 * j, 2)],
                send_sem=vs_send.at[0, j], recv_sem=vs_recv.at[0, j],
                device_id={"gx": lax.rem(gx + 1, n_gx), "gy": gy}, device_id_type=MESH,
            )

        def up_copy(j):
            return pltpu.make_async_remote_copy(
                src_ref=x_hbm.at[pl.ds(0, 1), pl.ds(2 * j, 2)],
                dst_ref=xp.at[pl.ds(rows + 1, 1), pl.ds(1 + 2 * j, 2)],
                send_sem=vs_send.at[1, j], recv_sem=vs_recv.at[1, j],
                device_id={"gx": lax.rem(gx + n_gx - 1, n_gx), "gy": gy}, device_id_type=MESH,
            )

        def right_copy(i):
            return pltpu.make_async_remote_copy(
                src_ref=x_hbm.at[pl.ds(2 * i, 2), pl.ds(cols - 1, 1)],
                dst_ref=xp.at[pl.ds(1 + 2 * i, 2), pl.ds(0, 1)],
                send_sem=hs_send.at[0, i], recv_sem=hs_recv.at[0, i],
                device_id={"gx": gx, "gy": lax.rem(gy + 1, n_gy)}, device_id_type=MESH,
            )

        def left_copy(i):
            return pltpu.make_async_remote_copy(
                src_ref=x_hbm.at[pl.ds(2 * i, 2), pl.ds(0, 1)],
                dst_ref=xp.at[pl.ds(1 + 2 * i, 2), pl.ds(cols + 1, 1)],
                send_sem=hs_send.at[1, i], recv_sem=hs_recv.at[1, i],
                device_id={"gx": gx, "gy": lax.rem(gy + n_gy - 1, n_gy)}, device_id_type=MESH,
            )

        v_order = list(range(1, bcols - 1)) + [0, bcols - 1]
        h_order = list(range(1, brows - 1)) + [0, brows - 1]
        def norms(r, c):
            values = xp[r, c].astype(F32)
            sq[r, c] = replicated_sum(values * values)

        for i in range(brows):
            loads[i].wait()

            def norm_pair(t, _, i=i):
                norms(1 + 2 * i, 1 + t)
                norms(2 + 2 * i, 1 + t)
                return 0

            lax.fori_loop(0, cols, norm_pair, 0)

        def arrive(bi, bj):
            @pl.when((bi == 0) & has_up)
            def _():
                down_copy(bj).wait_recv()
                norms(0, 1 + 2 * bj)
                norms(0, 2 + 2 * bj)

            @pl.when((bi == brows - 1) & has_down)
            def _():
                up_copy(bj).wait_recv()
                norms(rows + 1, 1 + 2 * bj)
                norms(rows + 1, 2 + 2 * bj)

            @pl.when((bj == 0) & has_left)
            def _():
                right_copy(bi).wait_recv()
                norms(1 + 2 * bi, 0)
                norms(2 + 2 * bi, 0)

            @pl.when((bj == bcols - 1) & has_right)
            def _():
                left_copy(bi).wait_recv()
                norms(1 + 2 * bi, cols + 1)
                norms(2 + 2 * bi, cols + 1)

        row8 = lax.broadcasted_iota(jnp.int32, (8, 256), 0)
        dims = (((1,), (0,)), ((), ()))
        dot = functools.partial(lax.dot_general, dimension_numbers=dims, preferred_element_type=F32)

        def stage_a(k, slot):
            bi, bj = self.block_of(k)
            r0, c0 = 1 + 2 * bi, 1 + 2 * bj
            at = lambda a, b: xp[r0 + a, c0 + b]
            own = [at(0, 0), at(0, 1), at(1, 0), at(1, 1)]
            q_rhs = jnp.concatenate(own, axis=0)
            qs[slot] = dot(jnp.concatenate([q_rhs.T, wq[...]], axis=0), q_rhs)

            def node(n):
                a, b = n // 2, n % 2
                va, hb = (-1, 2)[a], (-1, 2)[b]
                opposite, vert, horiz = own[3 - n], at(va, b), at(a, hb)
                total = (
                    (sq[r0 + a, c0 + b] + sq[r0 + va, c0 + b])
                    + (sq[r0 + a, c0 + hb] + sq[r0 + 1 - a, c0 + b])
                    + sq[r0 + a, c0 + 1 - b]
                )
                s1, s2, s3 = split3(total * -0.5)
                pick = lambda base, x: jnp.where(
                    row8 == x, s1, jnp.where(row8 == x + 1, s2, jnp.where(row8 == x + 2, s3, base[...]))
                )
                zeros8 = jnp.zeros((8, 256), F32)
                aug_r = jnp.concatenate([pick(base_r, 3), zeros8], axis=0).astype(BF16)
                aug_l = jnp.concatenate([pick(base_l, 0), zeros8], axis=0).astype(BF16)
                rhs = jnp.concatenate([opposite, vert, horiz, aug_r, hot[2 * bj + b]], axis=0)
                lhs_t = jnp.concatenate([-opposite, vert, horiz, aug_l, jnp.zeros((48, 256), BF16)], axis=0)
                weight = jnp.concatenate([wv[a], whb[2 * bi + a, b]], axis=1)
                rest = dot(jnp.concatenate([lhs_t.T, weight], axis=0), rhs)
                h = spread_ref[2 * bi + a, 2 * bj + b]
                kernel = jnp.exp2((qs[slot, 0:256] + rest[0:256]) * (2.0 * LOG2E / h))
                klow[slot, n] = kernel.astype(BF16)
                score = qs[slot, 256 + 64 * n : 320 + 64 * n] + rest[256:320]
                st[slot, n, 0:64] = score.astype(BF16)
                st[slot, n, 64:128] = own[n]

            return node

        def stage_c(k, slot):
            bi, bj = self.block_of(k)

            def node(n):
                a, b = n // 2, n % 2
                h = spread_ref[2 * bi + a, 2 * bj + b]
                scale = 2.0 / h
                prod = dot(st[slot, n], klow[slot, n])
                pull, push, colsum = prod[0:64], prod[64:128], prod[128:136]
                s = st[slot, n, 0:64].astype(F32)
                x = st[slot, n, 64:128].astype(F32)
                v = (push - x * jnp.concatenate([colsum] * 8, axis=0)) * scale
                force = pull - v
                fo[2 * bi + a, 2 * bj + b] = force.astype(BF16)
                acc[...] += row_fold(s * (force - v)) + (2.0 * scale) * row_fold(x * v) + (8.0 * scale) * colsum

            return node

        blocks = brows * bcols

        def pair_arrives(j):
            @pl.when(2 * j + 1 >= (brows - 2) * (bcols - 2))
            def _():
                def one(u, _):
                    arrive(*self.block_of(2 * j + u))
                    return 0

                lax.fori_loop(0, 2, one, 0)

        for slot in range(2):
            node = stage_a(slot, slot)
            for n in range(4):
                node(n)

        pl.semaphore_wait(barrier, n_gx + n_gy - 2)
        for off in range(1, n_gx):
            pl.semaphore_signal(
                ready, inc=1, device_id={"gx": lax.rem(gx + off, n_gx), "gy": gy}, device_id_type=MESH
            )

        @pl.when(has_down)
        def _():
            for j in v_order:
                down_copy(j).start()

        @pl.when(has_up)
        def _():
            for j in v_order:
                up_copy(j).start()

        @pl.when(has_right)
        def _():
            for i in h_order:
                right_copy(i).start()

        @pl.when(has_left)
        def _():
            for i in h_order:
                left_copy(i).start()

        unroll = 3

        def body(j, _):
            for u in range(unroll):
                pair_arrives(unroll * j + u + 1)
            for u in range(unroll):
                p = unroll * j + u
                for slot in range(2):
                    behind, ahead = stage_c(2 * p + slot, slot), stage_a(2 * p + 2 + slot, slot)
                    for n in range(4):
                        behind(n)
                        ahead(n)
            return 0

        lax.fori_loop(0, (blocks // 2 - 1) // unroll, body, 0)
        for slot in range(2):
            node = stage_c(blocks - 2 + slot, slot)
            for n in range(4):
                node(n)

        mine = jnp.sum(acc[:, 0:128] + acc[:, 128:256], axis=0, keepdims=True)
        me = gx * n_gy + gy
        ar_stage[0] = mine
        ar_all[me] = mine

        def ring(d, n):
            return min(d % n, n - d % n)

        def distance(off):
            z = (ring(off[0] // 2, n_gx // 2) + ring((off[0] + 1) // 2, n_gx // 2)) / 2
            y = (ring(off[1] // 4, 4) * (4 - off[1] % 4) + ring(off[1] // 4 + 1, 4) * (off[1] % 4)) / 4
            return z + y + ring(off[1], 4)

        offs = [(i, j) for i in range(n_gx) for j in range(n_gy) if i or j]
        offs.sort(key=distance, reverse=True)

        def sum_copy(t):
            i, j = offs[t]
            return pltpu.make_async_remote_copy(
                src_ref=ar_stage, dst_ref=ar_all.at[pl.ds(me, 1)], send_sem=ar_send.at[t], recv_sem=ar_recv.at[t],
                device_id={"gx": lax.rem(gx + i, n_gx), "gy": lax.rem(gy + j, n_gy)}, device_id_type=MESH,
            )

        pl.semaphore_wait(ready, n_gx - 1)
        for t in range(len(offs)):
            sum_copy(t).start()
        for t in range(len(offs)):
            sum_copy(t).wait_recv()
        pairs = float(rows * n_gx * cols * n_gy * 256 * 256)
        stein_ref[0, 0] = jnp.sum(ar_all[...]) / pairs

        for t in range(len(offs)):
            sum_copy(t).wait_send()

        @pl.when(has_down)
        def _():
            for j in v_order:
                down_copy(j).wait_send()

        @pl.when(has_up)
        def _():
            for j in v_order:
                up_copy(j).wait_send()

        @pl.when(has_right)
        def _():
            for i in h_order:
                right_copy(i).wait_send()

        @pl.when(has_left)
        def _():
            for i in h_order:
                left_copy(i).wait_send()


def solution(mesh):
    n_gx, n_gy = mesh.shape["gx"], mesh.shape["gy"]

    def step(particles, bias, spread, precision, coupling_h, coupling_v):
        rows, cols = particles.shape[:2]
        dma = pltpu.SemaphoreType.DMA
        hbm = pl.BlockSpec(memory_space=pltpu.HBM)
        smem = pl.BlockSpec(memory_space=pltpu.SMEM)
        force, stein = pl.pallas_call(
            Kernel(n_gx, n_gy, rows, cols),
            name="svgd",
            out_shape=(
                jax.ShapeDtypeStruct(particles.shape, BF16),
                jax.ShapeDtypeStruct((1, 1), F32),
            ),
            in_specs=[hbm] * 6,
            out_specs=(pl.BlockSpec(memory_space=pltpu.VMEM), smem),
            scratch_shapes=[
                pltpu.VMEM(bias.shape, F32),
                pltpu.SMEM(spread.shape, F32),
                pltpu.VMEM((64, 64), BF16),
                pltpu.VMEM((64, 64), BF16),
                pltpu.VMEM((64, 64), BF16),
                dma((5,)),
                pltpu.VMEM((rows + 2, cols + 2, 64, 256), BF16),
                pltpu.VMEM((rows + 2, cols + 2, 8, 256), F32),
                pltpu.VMEM((2, 4, 256, 256), BF16),
                pltpu.VMEM((2, 4, 144, 256), BF16),
                pltpu.VMEM((2, 512, 256), F32),
                pltpu.VMEM((cols, 48, 256), BF16),
                pltpu.VMEM((8, 256), F32),
                pltpu.VMEM((8, 256), F32),
                pltpu.VMEM((256, 256), BF16),
                pltpu.VMEM((2, 64, 128), BF16),
                pltpu.VMEM((rows, 2, 64, 128), BF16),
                pltpu.VMEM((8, 256), F32),
                pltpu.VMEM((1, 1, 128), F32),
                pltpu.VMEM((n_gx * n_gy, 1, 128), F32),
                dma((rows // 2,)),
                dma((2, rows // 2)),
                dma((2, rows // 2)),
                dma((2, cols // 2)),
                dma((2, cols // 2)),
                dma((n_gx * n_gy - 1,)),
                dma((n_gx * n_gy - 1,)),
                pltpu.SemaphoreType.REGULAR,
            ],
            compiler_params=pltpu.CompilerParams(collective_id=0, has_side_effects=True, vmem_limit_bytes=50_000_000),
        )(particles, *(pltpu.with_memory_space_constraint(v, pltpu.HBM) for v in (bias, spread, precision, coupling_h, coupling_v)))
        return force, stein[0, 0]

    return jax.shard_map(
        step,
        mesh=mesh,
        in_specs=(P("gx", "gy", None, None), P("gx", "gy", None), P("gx", "gy"), P(), P(), P()),
        out_specs=(P("gx", "gy", None, None), P()),
        check_vma=False,
    )
```

```python
import functools
import math

import jax
import jax.numpy as jnp
from jax import lax
from jax.experimental import pallas as pl
from jax.experimental.pallas import tpu as pltpu
from jax.sharding import PartitionSpec as P

MESH = pl.DeviceIdType.MESH
F32 = jnp.float32
BF16 = jnp.bfloat16
LOG2E = math.log2(math.e)


def row_fold(values):
    parts = [values[8 * i : 8 * i + 8] for i in range(values.shape[0] // 8)]
    while len(parts) > 1:
        parts = [a + b for a, b in zip(parts[::2], parts[1::2])]
    return parts[0]


def replicated_sum(values):
    folded = row_fold(values)
    return jnp.broadcast_to(jnp.sum(folded, axis=0, keepdims=True), folded.shape)


def top_bits(values):
    scaled = values * 65537.0
    return scaled - (scaled - values)


def split3(values):
    first = top_bits(values)
    rest = values - first
    second = top_bits(rest)
    return first, second, rest - second


class Kernel:
    def __init__(self, n_gx, n_gy, rows, cols):
        self.n_gx, self.n_gy, self.rows, self.cols = n_gx, n_gy, rows, cols
        self.brows, self.bcols = rows // 2, cols // 2

    def block_of(self, k):
        br, bc = self.brows, self.bcols
        inner = (br - 2) * (bc - 2)
        k1 = k - inner
        k2 = k1 - 2 * (bc - 2)
        k3 = k2 - 2 * (br - 2)
        where = lambda cond, a, b: lax.select(cond, jnp.int32(a), jnp.int32(b))
        k = jnp.int32(k)
        kk = jnp.maximum(jnp.int32(k), 0)
        k1 = jnp.maximum(jnp.int32(k1), 0)
        k2 = jnp.maximum(jnp.int32(k2), 0)
        k3 = jnp.maximum(jnp.int32(k3), 0)
        bi = where(k < inner, 1 + kk // (bc - 2), 0)
        bj = where(k < inner, 1 + kk % (bc - 2), 0)
        on1 = (k >= inner) & (k < inner + 2 * (bc - 2))
        bi = where(on1, (br - 1) * (k1 % 2), bi)
        bj = where(on1, 1 + k1 // 2, bj)
        on2 = (k >= inner + 2 * (bc - 2)) & (k < inner + 2 * (bc - 2) + 2 * (br - 2))
        bi = where(on2, 1 + k2 // 2, bi)
        bj = where(on2, (bc - 1) * (k2 % 2), bj)
        on3 = k >= inner + 2 * (bc - 2) + 2 * (br - 2)
        bi = where(on3, (br - 1) * (k3 // 2), bi)
        bj = where(on3, (bc - 1) * (k3 % 2), bj)
        return bi, bj

    def __call__(
        self, x_hbm, bias_hbm, spread_hbm, prec_hbm, ch_hbm, cv_hbm, fo, stein_ref,
        bias_ref, spread_ref, prec_ref, ch_ref, cv_ref, small_sem, xp, sq, klow, st, qs, hot, base_l, base_r, wq, wv, whb, acc, ar_stage, ar_all,
        load_sem, hs_send, hs_recv, vs_send, vs_recv, ar_send, ar_recv, ready,
    ):
        rows, cols, n_gx, n_gy = self.rows, self.cols, self.n_gx, self.n_gy
        brows, bcols = self.brows, self.bcols
        gx, gy = lax.axis_index("gx"), lax.axis_index("gy")

        loads = [
            pltpu.make_async_copy(
                x_hbm.at[pl.ds(2 * i, 2)], xp.at[pl.ds(1 + 2 * i, 2), pl.ds(1, cols)], load_sem.at[i]
            )
            for i in range(brows)
        ]
        smalls = [
            pltpu.make_async_copy(src, dst, small_sem.at[i])
            for i, (src, dst) in enumerate(
                [(prec_hbm, prec_ref), (ch_hbm, ch_ref), (cv_hbm, cv_ref), (bias_hbm, bias_ref), (spread_hbm, spread_ref)]
            )
        ]
        for copy in smalls + loads:
            copy.start()
        barrier = pltpu.get_barrier_semaphore()
        for off in range(1, n_gx):
            pl.semaphore_signal(
                barrier, inc=1, device_id={"gx": lax.rem(gx + off, n_gx), "gy": gy}, device_id_type=MESH
            )
        for off in range(1, n_gy):
            pl.semaphore_signal(
                barrier, inc=1, device_id={"gx": gx, "gy": lax.rem(gy + off, n_gy)}, device_id_type=MESH
            )

        for copy in smalls:
            copy.wait()
        minus_a = (-(prec_ref[...].astype(F32))).astype(BF16)
        h_mat, v_mat = ch_ref[...], cv_ref[...]
        h_t, v_t = h_mat.T, v_mat.T
        zero = jnp.zeros_like(h_mat)
        table = [
            [minus_a, h_mat, v_mat, zero],
            [h_t, minus_a, zero, v_mat],
            [v_t, zero, minus_a, h_mat],
            [zero, v_t, h_t, minus_a],
        ]
        for a in range(4):
            wq[64 * a : 64 * a + 64, :] = jnp.concatenate(table[a], axis=1)
        wv[0] = jnp.concatenate([zero, v_t], axis=1)
        wv[1] = jnp.concatenate([zero, v_mat], axis=1)
        for r in range(rows):
            parts = [p.astype(BF16) for p in split3(bias_ref[r])]
            tail = jnp.concatenate([jnp.zeros((16, 64), BF16)] + parts, axis=0)
            tail_t = tail.T
            whb[r, 0] = jnp.concatenate([h_t, tail_t], axis=1)
            whb[r, 1] = jnp.concatenate([h_mat, tail_t], axis=1)
        acc[...] = jnp.zeros_like(acc)
        row = lax.broadcasted_iota(jnp.int32, (8, 256), 0)
        for slot in range(2):
            for n in range(4):
                st[slot, n, 128:144] = jnp.ones((16, 256), BF16)
        base_r[...] = jnp.where(row < 3, 1.0, 0.0)
        base_l[...] = jnp.where((row >= 3) & (row < 6), 1.0, 0.0)
        hot_row = lax.broadcasted_iota(jnp.int32, (48, 256), 0) % 16

        def one_hot(col, _):
            hot[col] = jnp.where(hot_row == col, 1.0, 0.0).astype(BF16)
            return 0

        lax.fori_loop(0, cols, one_hot, 0)

        def clear(row, row_count, col, col_count):
            def one(t, _):
                r, c = row + t // col_count, col + t % col_count
                xp[r, c] = jnp.zeros((64, 256), BF16)
                sq[r, c] = jnp.zeros((8, 256), F32)
                return 0

            lax.fori_loop(0, row_count * col_count, one, 0)

        has_up, has_down = gx > 0, gx < n_gx - 1
        has_left, has_right = gy > 0, gy < n_gy - 1
        pl.when(jnp.logical_not(has_up))(lambda: clear(0, 1, 1, cols))
        pl.when(jnp.logical_not(has_down))(lambda: clear(rows + 1, 1, 1, cols))
        pl.when(jnp.logical_not(has_left))(lambda: clear(1, rows, 0, 1))
        pl.when(jnp.logical_not(has_right))(lambda: clear(1, rows, cols + 1, 1))

        def down_copy(j):
            return pltpu.make_async_remote_copy(
                src_ref=x_hbm.at[pl.ds(rows - 1, 1), pl.ds(2 * j, 2)],
                dst_ref=xp.at[pl.ds(0, 1), pl.ds(1 + 2 * j, 2)],
                send_sem=vs_send.at[0, j], recv_sem=vs_recv.at[0, j],
                device_id={"gx": lax.rem(gx + 1, n_gx), "gy": gy}, device_id_type=MESH,
            )

        def up_copy(j):
            return pltpu.make_async_remote_copy(
                src_ref=x_hbm.at[pl.ds(0, 1), pl.ds(2 * j, 2)],
                dst_ref=xp.at[pl.ds(rows + 1, 1), pl.ds(1 + 2 * j, 2)],
                send_sem=vs_send.at[1, j], recv_sem=vs_recv.at[1, j],
                device_id={"gx": lax.rem(gx + n_gx - 1, n_gx), "gy": gy}, device_id_type=MESH,
            )

        def right_copy(i):
            return pltpu.make_async_remote_copy(
                src_ref=x_hbm.at[pl.ds(2 * i, 2), pl.ds(cols - 1, 1)],
                dst_ref=xp.at[pl.ds(1 + 2 * i, 2), pl.ds(0, 1)],
                send_sem=hs_send.at[0, i], recv_sem=hs_recv.at[0, i],
                device_id={"gx": gx, "gy": lax.rem(gy + 1, n_gy)}, device_id_type=MESH,
            )

        def left_copy(i):
            return pltpu.make_async_remote_copy(
                src_ref=x_hbm.at[pl.ds(2 * i, 2), pl.ds(0, 1)],
                dst_ref=xp.at[pl.ds(1 + 2 * i, 2), pl.ds(cols + 1, 1)],
                send_sem=hs_send.at[1, i], recv_sem=hs_recv.at[1, i],
                device_id={"gx": gx, "gy": lax.rem(gy + n_gy - 1, n_gy)}, device_id_type=MESH,
            )

        v_order = list(range(1, bcols - 1)) + [0, bcols - 1]
        h_order = list(range(1, brows - 1)) + [0, brows - 1]
        def norms(r, c):
            values = xp[r, c].astype(F32)
            sq[r, c] = replicated_sum(values * values)

        for i in range(brows):
            loads[i].wait()

            def norm_group(t, _, i=i):
                for a in range(2):
                    for b in range(4):
                        norms(1 + 2 * i + a, 1 + 4 * t + b)
                return 0

            lax.fori_loop(0, cols // 4, norm_group, 0)

        def arrive(bi, bj):
            @pl.when((bi == 0) & has_up)
            def _():
                down_copy(bj).wait_recv()
                norms(0, 1 + 2 * bj)
                norms(0, 2 + 2 * bj)

            @pl.when((bi == brows - 1) & has_down)
            def _():
                up_copy(bj).wait_recv()
                norms(rows + 1, 1 + 2 * bj)
                norms(rows + 1, 2 + 2 * bj)

            @pl.when((bj == 0) & has_left)
            def _():
                right_copy(bi).wait_recv()
                norms(1 + 2 * bi, 0)
                norms(2 + 2 * bi, 0)

            @pl.when((bj == bcols - 1) & has_right)
            def _():
                left_copy(bi).wait_recv()
                norms(1 + 2 * bi, cols + 1)
                norms(2 + 2 * bi, cols + 1)

        row8 = lax.broadcasted_iota(jnp.int32, (8, 256), 0)
        dims = (((1,), (0,)), ((), ()))
        dot = functools.partial(lax.dot_general, dimension_numbers=dims, preferred_element_type=F32)

        def stage_a(k, slot):
            bi, bj = self.block_of(k)
            r0, c0 = 1 + 2 * bi, 1 + 2 * bj
            at = lambda a, b: xp[r0 + a, c0 + b]
            own = [at(0, 0), at(0, 1), at(1, 0), at(1, 1)]
            q_rhs = jnp.concatenate(own, axis=0)
            qs[slot] = dot(jnp.concatenate([q_rhs.T, wq[...]], axis=0), q_rhs)

            def node(n):
                a, b = n // 2, n % 2
                va, hb = (-1, 2)[a], (-1, 2)[b]
                opposite, vert, horiz = own[3 - n], at(va, b), at(a, hb)
                total = (
                    (sq[r0 + a, c0 + b] + sq[r0 + va, c0 + b])
                    + (sq[r0 + a, c0 + hb] + sq[r0 + 1 - a, c0 + b])
                    + sq[r0 + a, c0 + 1 - b]
                )
                s1, s2, s3 = split3(total * -0.5)
                pick = lambda base, x: jnp.where(
                    row8 == x, s1, jnp.where(row8 == x + 1, s2, jnp.where(row8 == x + 2, s3, base[...]))
                )
                zeros8 = jnp.zeros((8, 256), F32)
                aug_r = jnp.concatenate([pick(base_r, 3), zeros8], axis=0).astype(BF16)
                aug_l = jnp.concatenate([pick(base_l, 0), zeros8], axis=0).astype(BF16)
                rhs = jnp.concatenate([opposite, vert, horiz, aug_r, hot[2 * bj + b]], axis=0)
                lhs_t = jnp.concatenate([-opposite, vert, horiz, aug_l, jnp.zeros((48, 256), BF16)], axis=0)
                weight = jnp.concatenate([wv[a], whb[2 * bi + a, b]], axis=1)
                rest = dot(jnp.concatenate([lhs_t.T, weight], axis=0), rhs)
                h = spread_ref[2 * bi + a, 2 * bj + b]
                kernel = jnp.exp2((qs[slot, 0:256] + rest[0:256]) * (2.0 * LOG2E / h))
                klow[slot, n] = kernel.astype(BF16)
                score = qs[slot, 256 + 64 * n : 320 + 64 * n] + rest[256:320]
                st[slot, n, 0:64] = score.astype(BF16)
                st[slot, n, 64:128] = own[n]

            return node

        def stage_c(k, slot):
            bi, bj = self.block_of(k)

            def node(n):
                a, b = n // 2, n % 2
                h = spread_ref[2 * bi + a, 2 * bj + b]
                scale = 2.0 / h
                prod = dot(st[slot, n], klow[slot, n])
                pull, push, colsum = prod[0:64], prod[64:128], prod[128:136]
                s = st[slot, n, 0:64].astype(F32)
                x = st[slot, n, 64:128].astype(F32)
                v = (push - x * jnp.concatenate([colsum] * 8, axis=0)) * scale
                force = pull - v
                fo[2 * bi + a, 2 * bj + b] = force.astype(BF16)
                acc[...] += row_fold(s * (force - v)) + (2.0 * scale) * row_fold(x * v) + (8.0 * scale) * colsum

            return node

        blocks = brows * bcols

        def pair_arrives(j):
            @pl.when(2 * j + 1 >= (brows - 2) * (bcols - 2))
            def _():
                def one(u, _):
                    arrive(*self.block_of(2 * j + u))
                    return 0

                lax.fori_loop(0, 2, one, 0)

        pl.semaphore_wait(barrier, n_gx + n_gy - 2)
        for off in range(1, n_gx):
            pl.semaphore_signal(
                ready, inc=1, device_id={"gx": lax.rem(gx + off, n_gx), "gy": gy}, device_id_type=MESH
            )

        @pl.when(has_down)
        def _():
            for j in v_order:
                down_copy(j).start()

        @pl.when(has_up)
        def _():
            for j in v_order:
                up_copy(j).start()

        @pl.when(has_right)
        def _():
            for i in h_order:
                right_copy(i).start()

        @pl.when(has_left)
        def _():
            for i in h_order:
                left_copy(i).start()

        for slot in range(2):
            node = stage_a(slot, slot)
            for n in range(4):
                node(n)

        unroll = 3

        def body(j, _):
            for u in range(unroll):
                pair_arrives(unroll * j + u + 1)
            for u in range(unroll):
                p = unroll * j + u
                for slot in range(2):
                    behind, ahead = stage_c(2 * p + slot, slot), stage_a(2 * p + 2 + slot, slot)
                    for n in range(4):
                        behind(n)
                        ahead(n)
            return 0

        lax.fori_loop(0, (blocks // 2 - 1) // unroll, body, 0)
        for slot in range(2):
            node = stage_c(blocks - 2 + slot, slot)
            for n in range(4):
                node(n)

        mine = jnp.sum(acc[:, 0:128] + acc[:, 128:256], axis=0, keepdims=True)
        me = gx * n_gy + gy
        ar_stage[0] = mine
        ar_all[me] = mine

        def ring(d, n):
            return min(d % n, n - d % n)

        def distance(off):
            z = (ring(off[0] // 2, n_gx // 2) + ring((off[0] + 1) // 2, n_gx // 2)) / 2
            y = (ring(off[1] // 4, 4) * (4 - off[1] % 4) + ring(off[1] // 4 + 1, 4) * (off[1] % 4)) / 4
            return z + y + ring(off[1], 4)

        offs = [(i, j) for i in range(n_gx) for j in range(n_gy) if i or j]
        offs.sort(key=distance, reverse=True)

        def sum_copy(t):
            i, j = offs[t]
            return pltpu.make_async_remote_copy(
                src_ref=ar_stage, dst_ref=ar_all.at[pl.ds(me, 1)], send_sem=ar_send.at[t], recv_sem=ar_recv.at[t],
                device_id={"gx": lax.rem(gx + i, n_gx), "gy": lax.rem(gy + j, n_gy)}, device_id_type=MESH,
            )

        pl.semaphore_wait(ready, n_gx - 1)
        for t in range(len(offs)):
            sum_copy(t).start()
        for t in range(len(offs)):
            sum_copy(t).wait_send()

        @pl.when(has_down)
        def _():
            for j in v_order:
                down_copy(j).wait_send()

        @pl.when(has_up)
        def _():
            for j in v_order:
                up_copy(j).wait_send()

        @pl.when(has_right)
        def _():
            for i in h_order:
                right_copy(i).wait_send()

        @pl.when(has_left)
        def _():
            for i in h_order:
                left_copy(i).wait_send()

        for t in range(len(offs)):
            sum_copy(t).wait_recv()
        pairs = float(rows * n_gx * cols * n_gy * 256 * 256)
        stein_ref[0, 0] = jnp.sum(ar_all[...]) / pairs


def solution(mesh):
    n_gx, n_gy = mesh.shape["gx"], mesh.shape["gy"]

    def step(particles, bias, spread, precision, coupling_h, coupling_v):
        rows, cols = particles.shape[:2]
        dma = pltpu.SemaphoreType.DMA
        hbm = pl.BlockSpec(memory_space=pltpu.HBM)
        smem = pl.BlockSpec(memory_space=pltpu.SMEM)
        force, stein = pl.pallas_call(
            Kernel(n_gx, n_gy, rows, cols),
            name="svgd",
            out_shape=(
                jax.ShapeDtypeStruct(particles.shape, BF16),
                jax.ShapeDtypeStruct((1, 1), F32),
            ),
            in_specs=[hbm] * 6,
            out_specs=(pl.BlockSpec(memory_space=pltpu.VMEM), smem),
            scratch_shapes=[
                pltpu.VMEM(bias.shape, F32),
                pltpu.SMEM(spread.shape, F32),
                pltpu.VMEM((64, 64), BF16),
                pltpu.VMEM((64, 64), BF16),
                pltpu.VMEM((64, 64), BF16),
                dma((5,)),
                pltpu.VMEM((rows + 2, cols + 2, 64, 256), BF16),
                pltpu.VMEM((rows + 2, cols + 2, 8, 256), F32),
                pltpu.VMEM((2, 4, 256, 256), BF16),
                pltpu.VMEM((2, 4, 144, 256), BF16),
                pltpu.VMEM((2, 512, 256), F32),
                pltpu.VMEM((cols, 48, 256), BF16),
                pltpu.VMEM((8, 256), F32),
                pltpu.VMEM((8, 256), F32),
                pltpu.VMEM((256, 256), BF16),
                pltpu.VMEM((2, 64, 128), BF16),
                pltpu.VMEM((rows, 2, 64, 128), BF16),
                pltpu.VMEM((8, 256), F32),
                pltpu.VMEM((1, 1, 128), F32),
                pltpu.VMEM((n_gx * n_gy, 1, 128), F32),
                dma((rows // 2,)),
                dma((2, rows // 2)),
                dma((2, rows // 2)),
                dma((2, cols // 2)),
                dma((2, cols // 2)),
                dma((n_gx * n_gy - 1,)),
                dma((n_gx * n_gy - 1,)),
                pltpu.SemaphoreType.REGULAR,
            ],
            compiler_params=pltpu.CompilerParams(collective_id=0, has_side_effects=True, vmem_limit_bytes=50_000_000),
        )(particles, *(pltpu.with_memory_space_constraint(v, pltpu.HBM) for v in (bias, spread, precision, coupling_h, coupling_v)))
        return force, stein[0, 0]

    return jax.shard_map(
        step,
        mesh=mesh,
        in_specs=(P("gx", "gy", None, None), P("gx", "gy", None), P("gx", "gy"), P(), P(), P()),
        out_specs=(P("gx", "gy", None, None), P()),
        check_vma=False,
    )
```

```python
import functools
import math

import jax
import jax.numpy as jnp
from jax import lax
from jax.experimental import pallas as pl
from jax.experimental.pallas import tpu as pltpu
from jax.sharding import PartitionSpec as P

MESH = pl.DeviceIdType.MESH
F32 = jnp.float32
BF16 = jnp.bfloat16
LOG2E = math.log2(math.e)


def row_fold(values):
    parts = [values[8 * i : 8 * i + 8] for i in range(values.shape[0] // 8)]
    while len(parts) > 1:
        parts = [a + b for a, b in zip(parts[::2], parts[1::2])]
    return parts[0]


def replicated_sum(values):
    folded = row_fold(values)
    return jnp.broadcast_to(jnp.sum(folded, axis=0, keepdims=True), folded.shape)


def top_bits(values):
    scaled = values * 65537.0
    return scaled - (scaled - values)


def split3(values):
    first = top_bits(values)
    rest = values - first
    second = top_bits(rest)
    return first, second, rest - second


class Kernel:
    def __init__(self, n_gx, n_gy, rows, cols):
        self.n_gx, self.n_gy, self.rows, self.cols = n_gx, n_gy, rows, cols
        self.brows, self.bcols = rows // 2, cols // 2

    def block_of(self, k):
        br, bc = self.brows, self.bcols
        inner = (br - 2) * (bc - 2)
        k1 = k - inner
        k2 = k1 - 2 * (bc - 2)
        k3 = k2 - 2 * (br - 2)
        where = lambda cond, a, b: lax.select(cond, jnp.int32(a), jnp.int32(b))
        k = jnp.int32(k)
        kk = jnp.maximum(jnp.int32(k), 0)
        k1 = jnp.maximum(jnp.int32(k1), 0)
        k2 = jnp.maximum(jnp.int32(k2), 0)
        k3 = jnp.maximum(jnp.int32(k3), 0)
        bi = where(k < inner, 1 + kk // (bc - 2), 0)
        bj = where(k < inner, 1 + kk % (bc - 2), 0)
        on1 = (k >= inner) & (k < inner + 2 * (bc - 2))
        bi = where(on1, (br - 1) * (k1 % 2), bi)
        bj = where(on1, 1 + k1 // 2, bj)
        on2 = (k >= inner + 2 * (bc - 2)) & (k < inner + 2 * (bc - 2) + 2 * (br - 2))
        bi = where(on2, 1 + k2 // 2, bi)
        bj = where(on2, (bc - 1) * (k2 % 2), bj)
        on3 = k >= inner + 2 * (bc - 2) + 2 * (br - 2)
        bi = where(on3, (br - 1) * (k3 // 2), bi)
        bj = where(on3, (bc - 1) * (k3 % 2), bj)
        return bi, bj

    def fixed_block(self, k):
        br, bc = self.brows, self.bcols
        order = [(i, j) for i in range(1, br - 1) for j in range(1, bc - 1)]
        order += [(i, j) for j in range(1, bc - 1) for i in (0, br - 1)]
        order += [(i, j) for i in range(1, br - 1) for j in (0, bc - 1)]
        order += [(i, j) for i in (0, br - 1) for j in (0, bc - 1)]
        return order[k]

    def __call__(
        self, x_hbm, bias_hbm, spread_hbm, prec_hbm, ch_hbm, cv_hbm, fo, stein_ref,
        bias_ref, spread_ref, prec_ref, ch_ref, cv_ref, small_sem, xp, sq, klow, st, qs, hot, base_l, base_r, wq, wv, whb, acc, ar_stage, ar_all,
        load_sem, hs_send, hs_recv, vs_send, vs_recv, ar_send, ar_recv, ready,
    ):
        rows, cols, n_gx, n_gy = self.rows, self.cols, self.n_gx, self.n_gy
        brows, bcols = self.brows, self.bcols
        gx, gy = lax.axis_index("gx"), lax.axis_index("gy")

        loads = [
            pltpu.make_async_copy(
                x_hbm.at[pl.ds(2 * i, 2)], xp.at[pl.ds(1 + 2 * i, 2), pl.ds(1, cols)], load_sem.at[i]
            )
            for i in range(brows)
        ]
        smalls = [
            pltpu.make_async_copy(src, dst, small_sem.at[i])
            for i, (src, dst) in enumerate(
                [(prec_hbm, prec_ref), (ch_hbm, ch_ref), (cv_hbm, cv_ref), (bias_hbm, bias_ref), (spread_hbm, spread_ref)]
            )
        ]
        for copy in smalls + loads:
            copy.start()
        barrier = pltpu.get_barrier_semaphore()
        for off in range(1, n_gx):
            pl.semaphore_signal(
                barrier, inc=1, device_id={"gx": lax.rem(gx + off, n_gx), "gy": gy}, device_id_type=MESH
            )
        for off in range(1, n_gy):
            pl.semaphore_signal(
                barrier, inc=1, device_id={"gx": gx, "gy": lax.rem(gy + off, n_gy)}, device_id_type=MESH
            )

        for copy in smalls:
            copy.wait()
        minus_a = (-(prec_ref[...].astype(F32))).astype(BF16)
        h_mat, v_mat = ch_ref[...], cv_ref[...]
        h_t, v_t = h_mat.T, v_mat.T
        zero = jnp.zeros_like(h_mat)
        table = [
            [minus_a, h_mat, v_mat, zero],
            [h_t, minus_a, zero, v_mat],
            [v_t, zero, minus_a, h_mat],
            [zero, v_t, h_t, minus_a],
        ]
        for a in range(4):
            wq[64 * a : 64 * a + 64, :] = jnp.concatenate(table[a], axis=1)
        wv[0] = jnp.concatenate([zero, v_t], axis=1)
        wv[1] = jnp.concatenate([zero, v_mat], axis=1)
        for r in range(rows):
            parts = [p.astype(BF16) for p in split3(bias_ref[r])]
            tail = jnp.concatenate([jnp.zeros((16, 64), BF16)] + parts, axis=0)
            tail_t = tail.T
            whb[r, 0] = jnp.concatenate([h_t, tail_t], axis=1)
            whb[r, 1] = jnp.concatenate([h_mat, tail_t], axis=1)
        acc[...] = jnp.zeros_like(acc)
        row = lax.broadcasted_iota(jnp.int32, (8, 256), 0)
        for slot in range(2):
            for n in range(4):
                st[slot, n, 128:144] = jnp.ones((16, 256), BF16)
        base_r[...] = jnp.where(row < 3, 1.0, 0.0)
        base_l[...] = jnp.where((row >= 3) & (row < 6), 1.0, 0.0)
        hot_row = lax.broadcasted_iota(jnp.int32, (48, 256), 0) % 16

        def one_hot(col, _):
            hot[col] = jnp.where(hot_row == col, 1.0, 0.0).astype(BF16)
            return 0

        lax.fori_loop(0, cols, one_hot, 0)

        def clear(row, row_count, col, col_count):
            def one(t, _):
                r, c = row + t // col_count, col + t % col_count
                xp[r, c] = jnp.zeros((64, 256), BF16)
                return 0

            lax.fori_loop(0, row_count * col_count, one, 0)

        has_up, has_down = gx > 0, gx < n_gx - 1
        has_left, has_right = gy > 0, gy < n_gy - 1
        pl.when(jnp.logical_not(has_up))(lambda: clear(0, 1, 1, cols))
        pl.when(jnp.logical_not(has_down))(lambda: clear(rows + 1, 1, 1, cols))
        pl.when(jnp.logical_not(has_left))(lambda: clear(1, rows, 0, 1))
        pl.when(jnp.logical_not(has_right))(lambda: clear(1, rows, cols + 1, 1))

        def down_copy(j):
            return pltpu.make_async_remote_copy(
                src_ref=x_hbm.at[pl.ds(rows - 1, 1), pl.ds(2 * j, 2)],
                dst_ref=xp.at[pl.ds(0, 1), pl.ds(1 + 2 * j, 2)],
                send_sem=vs_send.at[0, j], recv_sem=vs_recv.at[0, j],
                device_id={"gx": lax.rem(gx + 1, n_gx), "gy": gy}, device_id_type=MESH,
            )

        def up_copy(j):
            return pltpu.make_async_remote_copy(
                src_ref=x_hbm.at[pl.ds(0, 1), pl.ds(2 * j, 2)],
                dst_ref=xp.at[pl.ds(rows + 1, 1), pl.ds(1 + 2 * j, 2)],
                send_sem=vs_send.at[1, j], recv_sem=vs_recv.at[1, j],
                device_id={"gx": lax.rem(gx + n_gx - 1, n_gx), "gy": gy}, device_id_type=MESH,
            )

        def right_copy(i):
            return pltpu.make_async_remote_copy(
                src_ref=x_hbm.at[pl.ds(2 * i, 2), pl.ds(cols - 1, 1)],
                dst_ref=xp.at[pl.ds(1 + 2 * i, 2), pl.ds(0, 1)],
                send_sem=hs_send.at[0, i], recv_sem=hs_recv.at[0, i],
                device_id={"gx": gx, "gy": lax.rem(gy + 1, n_gy)}, device_id_type=MESH,
            )

        def left_copy(i):
            return pltpu.make_async_remote_copy(
                src_ref=x_hbm.at[pl.ds(2 * i, 2), pl.ds(0, 1)],
                dst_ref=xp.at[pl.ds(1 + 2 * i, 2), pl.ds(cols + 1, 1)],
                send_sem=hs_send.at[1, i], recv_sem=hs_recv.at[1, i],
                device_id={"gx": gx, "gy": lax.rem(gy + n_gy - 1, n_gy)}, device_id_type=MESH,
            )

        v_order = list(range(1, bcols - 1)) + [0, bcols - 1]
        h_order = list(range(1, brows - 1)) + [0, brows - 1]
        def norms(r, c):
            values = xp[r, c].astype(F32)
            sq[r, c] = replicated_sum(values * values)

        for i in range(brows):
            loads[i].wait()

            def norm_group(t, _, i=i):
                for a in range(2):
                    for b in range(4):
                        norms(1 + 2 * i + a, 1 + 4 * t + b)
                return 0

            lax.fori_loop(0, cols // 4, norm_group, 0)

        def arrivals(first, last):
            halo = []
            for k in range(first, last):
                bi, bj = self.fixed_block(k)
                if bi == 0:
                    pl.when(has_up)(lambda bj=bj: down_copy(bj).wait_recv())
                    halo += [(0, 1 + 2 * bj), (0, 2 + 2 * bj)]
                if bi == brows - 1:
                    pl.when(has_down)(lambda bj=bj: up_copy(bj).wait_recv())
                    halo += [(rows + 1, 1 + 2 * bj), (rows + 1, 2 + 2 * bj)]
                if bj == 0:
                    pl.when(has_left)(lambda bi=bi: right_copy(bi).wait_recv())
                    halo += [(1 + 2 * bi, 0), (2 + 2 * bi, 0)]
                if bj == bcols - 1:
                    pl.when(has_right)(lambda bi=bi: left_copy(bi).wait_recv())
                    halo += [(1 + 2 * bi, cols + 1), (2 + 2 * bi, cols + 1)]
            for r, c in halo:
                norms(r, c)

        row8 = lax.broadcasted_iota(jnp.int32, (8, 256), 0)
        dims = (((1,), (0,)), ((), ()))
        dot = functools.partial(lax.dot_general, dimension_numbers=dims, preferred_element_type=F32)

        def stage_a(k, slot):
            bi, bj = self.block_of(k)
            r0, c0 = 1 + 2 * bi, 1 + 2 * bj
            at = lambda a, b: xp[r0 + a, c0 + b]
            own = [at(0, 0), at(0, 1), at(1, 0), at(1, 1)]
            q_rhs = jnp.concatenate(own, axis=0)
            qs[slot] = dot(jnp.concatenate([q_rhs.T, wq[...]], axis=0), q_rhs)

            def node(n):
                a, b = n // 2, n % 2
                va, hb = (-1, 2)[a], (-1, 2)[b]
                opposite, vert, horiz = own[3 - n], at(va, b), at(a, hb)
                total = (
                    (sq[r0 + a, c0 + b] + sq[r0 + va, c0 + b])
                    + (sq[r0 + a, c0 + hb] + sq[r0 + 1 - a, c0 + b])
                    + sq[r0 + a, c0 + 1 - b]
                )
                s1, s2, s3 = split3(total * -0.5)
                pick = lambda base, x: jnp.where(
                    row8 == x, s1, jnp.where(row8 == x + 1, s2, jnp.where(row8 == x + 2, s3, base[...]))
                )
                zeros8 = jnp.zeros((8, 256), F32)
                aug_r = jnp.concatenate([pick(base_r, 3), zeros8], axis=0).astype(BF16)
                aug_l = jnp.concatenate([pick(base_l, 0), zeros8], axis=0).astype(BF16)
                rhs = jnp.concatenate([opposite, vert, horiz, aug_r, hot[2 * bj + b]], axis=0)
                lhs_t = jnp.concatenate([-opposite, vert, horiz, aug_l, jnp.zeros((48, 256), BF16)], axis=0)
                weight = jnp.concatenate([wv[a], whb[2 * bi + a, b]], axis=1)
                rest = dot(jnp.concatenate([lhs_t.T, weight], axis=0), rhs)
                h = spread_ref[2 * bi + a, 2 * bj + b]
                kernel = jnp.exp2((qs[slot, 0:256] + rest[0:256]) * (2.0 * LOG2E / h))
                klow[slot, n] = kernel.astype(BF16)
                score = qs[slot, 256 + 64 * n : 320 + 64 * n] + rest[256:320]
                st[slot, n, 0:64] = score.astype(BF16)
                st[slot, n, 64:128] = own[n]

            return node

        def stage_c(k, slot):
            bi, bj = self.block_of(k)

            def node(n):
                a, b = n // 2, n % 2
                h = spread_ref[2 * bi + a, 2 * bj + b]
                scale = 2.0 / h
                prod = dot(st[slot, n], klow[slot, n])
                pull, push, colsum = prod[0:64], prod[64:128], prod[128:136]
                s = st[slot, n, 0:64].astype(F32)
                x = st[slot, n, 64:128].astype(F32)
                v = (push - x * jnp.concatenate([colsum] * 8, axis=0)) * scale
                force = pull - v
                fo[2 * bi + a, 2 * bj + b] = force.astype(BF16)
                acc[...] += row_fold(s * (force - v)) + (2.0 * scale) * row_fold(x * v) + (8.0 * scale) * colsum

            return node

        blocks = brows * bcols

        pl.semaphore_wait(barrier, n_gx + n_gy - 2)
        for off in range(1, n_gx):
            pl.semaphore_signal(
                ready, inc=1, device_id={"gx": lax.rem(gx + off, n_gx), "gy": gy}, device_id_type=MESH
            )

        @pl.when(has_down)
        def _():
            for j in v_order:
                down_copy(j).start()

        @pl.when(has_up)
        def _():
            for j in v_order:
                up_copy(j).start()

        @pl.when(has_right)
        def _():
            for i in h_order:
                right_copy(i).start()

        @pl.when(has_left)
        def _():
            for i in h_order:
                left_copy(i).start()

        for slot in range(2):
            node = stage_a(slot, slot)
            for n in range(4):
                node(n)

        unroll = 3
        steps = (blocks // 2 - 1) // unroll
        inner = (brows - 2) * (bcols - 2)

        def body(j, _):
            for step in range(steps):
                first = 2 * (unroll * step + 1)
                if first + 2 * unroll > inner:
                    pl.when(j == step)(functools.partial(arrivals, max(first, inner), first + 2 * unroll))
            for u in range(unroll):
                p = unroll * j + u
                for slot in range(2):
                    behind, ahead = stage_c(2 * p + slot, slot), stage_a(2 * p + 2 + slot, slot)
                    for n in range(4):
                        behind(n)
                        ahead(n)
            return 0

        lax.fori_loop(0, steps, body, 0)
        for slot in range(2):
            node = stage_c(blocks - 2 + slot, slot)
            for n in range(4):
                node(n)

        mine = jnp.sum(acc[:, 0:128] + acc[:, 128:256], axis=0, keepdims=True)
        me = gx * n_gy + gy
        ar_stage[0] = mine
        ar_all[me] = mine

        def ring(d, n):
            return min(d % n, n - d % n)

        def distance(off):
            z = (ring(off[0] // 2, n_gx // 2) + ring((off[0] + 1) // 2, n_gx // 2)) / 2
            y = (ring(off[1] // 4, 4) * (4 - off[1] % 4) + ring(off[1] // 4 + 1, 4) * (off[1] % 4)) / 4
            return z + y + ring(off[1], 4)

        offs = [(i, j) for i in range(n_gx) for j in range(n_gy) if i or j]
        offs.sort(key=distance, reverse=True)

        def sum_copy(t):
            i, j = offs[t]
            return pltpu.make_async_remote_copy(
                src_ref=ar_stage, dst_ref=ar_all.at[pl.ds(me, 1)], send_sem=ar_send.at[t], recv_sem=ar_recv.at[t],
                device_id={"gx": lax.rem(gx + i, n_gx), "gy": lax.rem(gy + j, n_gy)}, device_id_type=MESH,
            )

        pl.semaphore_wait(ready, n_gx - 1)
        for t in range(len(offs)):
            sum_copy(t).start()
        for t in range(len(offs)):
            sum_copy(t).wait_send()

        @pl.when(has_down)
        def _():
            for j in v_order:
                down_copy(j).wait_send()

        @pl.when(has_up)
        def _():
            for j in v_order:
                up_copy(j).wait_send()

        @pl.when(has_right)
        def _():
            for i in h_order:
                right_copy(i).wait_send()

        @pl.when(has_left)
        def _():
            for i in h_order:
                left_copy(i).wait_send()

        for t in range(len(offs)):
            sum_copy(t).wait_recv()
        pairs = float(rows * n_gx * cols * n_gy * 256 * 256)
        stein_ref[0, 0] = jnp.sum(ar_all[...]) / pairs


def solution(mesh):
    n_gx, n_gy = mesh.shape["gx"], mesh.shape["gy"]

    def step(particles, bias, spread, precision, coupling_h, coupling_v):
        rows, cols = particles.shape[:2]
        dma = pltpu.SemaphoreType.DMA
        hbm = pl.BlockSpec(memory_space=pltpu.HBM)
        smem = pl.BlockSpec(memory_space=pltpu.SMEM)
        force, stein = pl.pallas_call(
            Kernel(n_gx, n_gy, rows, cols),
            name="svgd",
            out_shape=(
                jax.ShapeDtypeStruct(particles.shape, BF16),
                jax.ShapeDtypeStruct((1, 1), F32),
            ),
            in_specs=[hbm] * 6,
            out_specs=(pl.BlockSpec(memory_space=pltpu.VMEM), smem),
            scratch_shapes=[
                pltpu.VMEM(bias.shape, F32),
                pltpu.SMEM(spread.shape, F32),
                pltpu.VMEM((64, 64), BF16),
                pltpu.VMEM((64, 64), BF16),
                pltpu.VMEM((64, 64), BF16),
                dma((5,)),
                pltpu.VMEM((rows + 2, cols + 2, 64, 256), BF16),
                pltpu.VMEM((rows + 2, cols + 2, 8, 256), F32),
                pltpu.VMEM((2, 4, 256, 256), BF16),
                pltpu.VMEM((2, 4, 144, 256), BF16),
                pltpu.VMEM((2, 512, 256), F32),
                pltpu.VMEM((cols, 48, 256), BF16),
                pltpu.VMEM((8, 256), F32),
                pltpu.VMEM((8, 256), F32),
                pltpu.VMEM((256, 256), BF16),
                pltpu.VMEM((2, 64, 128), BF16),
                pltpu.VMEM((rows, 2, 64, 128), BF16),
                pltpu.VMEM((8, 256), F32),
                pltpu.VMEM((1, 1, 128), F32),
                pltpu.VMEM((n_gx * n_gy, 1, 128), F32),
                dma((rows // 2,)),
                dma((2, rows // 2)),
                dma((2, rows // 2)),
                dma((2, cols // 2)),
                dma((2, cols // 2)),
                dma((n_gx * n_gy - 1,)),
                dma((n_gx * n_gy - 1,)),
                pltpu.SemaphoreType.REGULAR,
            ],
            compiler_params=pltpu.CompilerParams(collective_id=0, has_side_effects=True, vmem_limit_bytes=50_000_000),
        )(particles, *(pltpu.with_memory_space_constraint(v, pltpu.HBM) for v in (bias, spread, precision, coupling_h, coupling_v)))
        return force, stein[0, 0]

    return jax.shard_map(
        step,
        mesh=mesh,
        in_specs=(P("gx", "gy", None, None), P("gx", "gy", None), P("gx", "gy"), P(), P(), P()),
        out_specs=(P("gx", "gy", None, None), P()),
        check_vma=False,
    )
```

```python
import functools
import math

import jax
import jax.numpy as jnp
from jax import lax
from jax.experimental import pallas as pl
from jax.experimental.pallas import tpu as pltpu
from jax.sharding import PartitionSpec as P

MESH = pl.DeviceIdType.MESH
F32 = jnp.float32
BF16 = jnp.bfloat16
LOG2E = math.log2(math.e)


def row_fold(values):
    parts = [values[8 * i : 8 * i + 8] for i in range(values.shape[0] // 8)]
    while len(parts) > 1:
        parts = [a + b for a, b in zip(parts[::2], parts[1::2])]
    return parts[0]


def replicated_sum(values):
    folded = row_fold(values)
    return jnp.broadcast_to(jnp.sum(folded, axis=0, keepdims=True), folded.shape)


def top_bits(values):
    scaled = values * 65537.0
    return scaled - (scaled - values)


def split3(values):
    first = top_bits(values)
    rest = values - first
    second = top_bits(rest)
    return first, second, rest - second


class Kernel:
    def __init__(self, n_gx, n_gy, rows, cols):
        self.n_gx, self.n_gy, self.rows, self.cols = n_gx, n_gy, rows, cols
        self.brows, self.bcols = rows // 2, cols // 2

    def block_of(self, k):
        br, bc = self.brows, self.bcols
        inner = (br - 2) * (bc - 2)
        k1 = k - inner
        k2 = k1 - 2 * (bc - 2)
        k3 = k2 - 2 * (br - 2)
        where = lambda cond, a, b: lax.select(cond, jnp.int32(a), jnp.int32(b))
        k = jnp.int32(k)
        kk = jnp.maximum(jnp.int32(k), 0)
        k1 = jnp.maximum(jnp.int32(k1), 0)
        k2 = jnp.maximum(jnp.int32(k2), 0)
        k3 = jnp.maximum(jnp.int32(k3), 0)
        bi = where(k < inner, 1 + kk // (bc - 2), 0)
        bj = where(k < inner, 1 + kk % (bc - 2), 0)
        on1 = (k >= inner) & (k < inner + 2 * (bc - 2))
        bi = where(on1, (br - 1) * (k1 % 2), bi)
        bj = where(on1, 1 + k1 // 2, bj)
        on2 = (k >= inner + 2 * (bc - 2)) & (k < inner + 2 * (bc - 2) + 2 * (br - 2))
        bi = where(on2, 1 + k2 // 2, bi)
        bj = where(on2, (bc - 1) * (k2 % 2), bj)
        on3 = k >= inner + 2 * (bc - 2) + 2 * (br - 2)
        bi = where(on3, (br - 1) * (k3 // 2), bi)
        bj = where(on3, (bc - 1) * (k3 % 2), bj)
        return bi, bj

    def fixed_block(self, k):
        br, bc = self.brows, self.bcols
        order = [(i, j) for i in range(1, br - 1) for j in range(1, bc - 1)]
        order += [(i, j) for j in range(1, bc - 1) for i in (0, br - 1)]
        order += [(i, j) for i in range(1, br - 1) for j in (0, bc - 1)]
        order += [(i, j) for i in (0, br - 1) for j in (0, bc - 1)]
        return order[k]

    def __call__(
        self, x_hbm, bias_hbm, spread_hbm, prec_hbm, ch_hbm, cv_hbm, fo, stein_ref,
        bias_ref, spread_ref, prec_ref, ch_ref, cv_ref, small_sem, xp, sq, klow, st, qs, hot, base_l, base_r, wq, wv, whb, acc, ar_stage, ar_all,
        load_sem, hs_send, hs_recv, vs_send, vs_recv, ar_send, ar_recv, ready,
    ):
        rows, cols, n_gx, n_gy = self.rows, self.cols, self.n_gx, self.n_gy
        brows, bcols = self.brows, self.bcols
        gx, gy = lax.axis_index("gx"), lax.axis_index("gy")

        loads = [
            pltpu.make_async_copy(
                x_hbm.at[pl.ds(2 * i, 2)], xp.at[pl.ds(1 + 2 * i, 2), pl.ds(1, cols)], load_sem.at[i]
            )
            for i in range(brows)
        ]
        smalls = [
            pltpu.make_async_copy(src, dst, small_sem.at[i])
            for i, (src, dst) in enumerate(
                [(prec_hbm, prec_ref), (ch_hbm, ch_ref), (cv_hbm, cv_ref), (bias_hbm, bias_ref), (spread_hbm, spread_ref)]
            )
        ]
        for copy in smalls + loads:
            copy.start()
        barrier = pltpu.get_barrier_semaphore()
        for off in range(1, n_gx):
            pl.semaphore_signal(
                barrier, inc=1, device_id={"gx": lax.rem(gx + off, n_gx), "gy": gy}, device_id_type=MESH
            )
        for off in range(1, n_gy):
            pl.semaphore_signal(
                barrier, inc=1, device_id={"gx": gx, "gy": lax.rem(gy + off, n_gy)}, device_id_type=MESH
            )

        acc[...] = jnp.zeros_like(acc)
        row = lax.broadcasted_iota(jnp.int32, (8, 256), 0)
        for slot in range(2):
            for n in range(4):
                st[slot, n, 128:144] = jnp.ones((16, 256), BF16)
        base_r[...] = jnp.where(row < 3, 1.0, 0.0)
        base_l[...] = jnp.where((row >= 3) & (row < 6), 1.0, 0.0)
        hot_row = lax.broadcasted_iota(jnp.int32, (48, 256), 0) % 16

        def one_hot(col, _):
            hot[col] = jnp.where(hot_row == col, 1.0, 0.0).astype(BF16)
            return 0

        lax.fori_loop(0, cols, one_hot, 0)

        def clear(row, row_count, col, col_count):
            def one(t, _):
                r, c = row + t // col_count, col + t % col_count
                xp[r, c] = jnp.zeros((64, 256), BF16)
                return 0

            lax.fori_loop(0, row_count * col_count, one, 0)

        has_up, has_down = gx > 0, gx < n_gx - 1
        has_left, has_right = gy > 0, gy < n_gy - 1
        pl.when(jnp.logical_not(has_up))(lambda: clear(0, 1, 1, cols))
        pl.when(jnp.logical_not(has_down))(lambda: clear(rows + 1, 1, 1, cols))
        pl.when(jnp.logical_not(has_left))(lambda: clear(1, rows, 0, 1))
        pl.when(jnp.logical_not(has_right))(lambda: clear(1, rows, cols + 1, 1))

        for copy in smalls:
            copy.wait()
        minus_a = (-(prec_ref[...].astype(F32))).astype(BF16)
        h_mat, v_mat = ch_ref[...], cv_ref[...]
        h_t, v_t = h_mat.T, v_mat.T
        zero = jnp.zeros_like(h_mat)
        table = [
            [minus_a, h_mat, v_mat, zero],
            [h_t, minus_a, zero, v_mat],
            [v_t, zero, minus_a, h_mat],
            [zero, v_t, h_t, minus_a],
        ]
        for a in range(4):
            wq[64 * a : 64 * a + 64, :] = jnp.concatenate(table[a], axis=1)
        wv[0] = jnp.concatenate([zero, v_t], axis=1)
        wv[1] = jnp.concatenate([zero, v_mat], axis=1)
        for r in range(rows):
            parts = [p.astype(BF16) for p in split3(bias_ref[r])]
            tail = jnp.concatenate([jnp.zeros((16, 64), BF16)] + parts, axis=0)
            tail_t = tail.T
            whb[r, 0] = jnp.concatenate([h_t, tail_t], axis=1)
            whb[r, 1] = jnp.concatenate([h_mat, tail_t], axis=1)

        def down_copy(j):
            return pltpu.make_async_remote_copy(
                src_ref=x_hbm.at[pl.ds(rows - 1, 1), pl.ds(2 * j, 2)],
                dst_ref=xp.at[pl.ds(0, 1), pl.ds(1 + 2 * j, 2)],
                send_sem=vs_send.at[0, j], recv_sem=vs_recv.at[0, j],
                device_id={"gx": lax.rem(gx + 1, n_gx), "gy": gy}, device_id_type=MESH,
            )

        def up_copy(j):
            return pltpu.make_async_remote_copy(
                src_ref=x_hbm.at[pl.ds(0, 1), pl.ds(2 * j, 2)],
                dst_ref=xp.at[pl.ds(rows + 1, 1), pl.ds(1 + 2 * j, 2)],
                send_sem=vs_send.at[1, j], recv_sem=vs_recv.at[1, j],
                device_id={"gx": lax.rem(gx + n_gx - 1, n_gx), "gy": gy}, device_id_type=MESH,
            )

        def right_copy(i):
            return pltpu.make_async_remote_copy(
                src_ref=x_hbm.at[pl.ds(2 * i, 2), pl.ds(cols - 1, 1)],
                dst_ref=xp.at[pl.ds(1 + 2 * i, 2), pl.ds(0, 1)],
                send_sem=hs_send.at[0, i], recv_sem=hs_recv.at[0, i],
                device_id={"gx": gx, "gy": lax.rem(gy + 1, n_gy)}, device_id_type=MESH,
            )

        def left_copy(i):
            return pltpu.make_async_remote_copy(
                src_ref=x_hbm.at[pl.ds(2 * i, 2), pl.ds(0, 1)],
                dst_ref=xp.at[pl.ds(1 + 2 * i, 2), pl.ds(cols + 1, 1)],
                send_sem=hs_send.at[1, i], recv_sem=hs_recv.at[1, i],
                device_id={"gx": gx, "gy": lax.rem(gy + n_gy - 1, n_gy)}, device_id_type=MESH,
            )

        v_order = list(range(1, bcols - 1)) + [0, bcols - 1]
        h_order = list(range(1, brows - 1)) + [0, brows - 1]
        def norms(r, c):
            values = xp[r, c].astype(F32)
            sq[r, c] = replicated_sum(values * values)

        for i in range(brows):
            loads[i].wait()

            def norm_group(t, _, i=i):
                for a in range(2):
                    for b in range(4):
                        norms(1 + 2 * i + a, 1 + 4 * t + b)
                return 0

            lax.fori_loop(0, cols // 4, norm_group, 0)

        def arrivals(first, last):
            halo = []
            for k in range(first, last):
                bi, bj = self.fixed_block(k)
                if bi == 0:
                    pl.when(has_up)(lambda bj=bj: down_copy(bj).wait_recv())
                    halo += [(0, 1 + 2 * bj), (0, 2 + 2 * bj)]
                if bi == brows - 1:
                    pl.when(has_down)(lambda bj=bj: up_copy(bj).wait_recv())
                    halo += [(rows + 1, 1 + 2 * bj), (rows + 1, 2 + 2 * bj)]
                if bj == 0:
                    pl.when(has_left)(lambda bi=bi: right_copy(bi).wait_recv())
                    halo += [(1 + 2 * bi, 0), (2 + 2 * bi, 0)]
                if bj == bcols - 1:
                    pl.when(has_right)(lambda bi=bi: left_copy(bi).wait_recv())
                    halo += [(1 + 2 * bi, cols + 1), (2 + 2 * bi, cols + 1)]
            for r, c in halo:
                norms(r, c)

        row8 = lax.broadcasted_iota(jnp.int32, (8, 256), 0)
        dims = (((1,), (0,)), ((), ()))
        dot = functools.partial(lax.dot_general, dimension_numbers=dims, preferred_element_type=F32)

        def stage_a(k, slot):
            bi, bj = self.block_of(k)
            r0, c0 = 1 + 2 * bi, 1 + 2 * bj
            at = lambda a, b: xp[r0 + a, c0 + b]
            own = [at(0, 0), at(0, 1), at(1, 0), at(1, 1)]
            q_rhs = jnp.concatenate(own, axis=0)
            qs[slot] = dot(jnp.concatenate([q_rhs.T, wq[...]], axis=0), q_rhs)

            def node(n):
                a, b = n // 2, n % 2
                va, hb = (-1, 2)[a], (-1, 2)[b]
                opposite, vert, horiz = own[3 - n], at(va, b), at(a, hb)
                total = (
                    (sq[r0 + a, c0 + b] + sq[r0 + va, c0 + b])
                    + (sq[r0 + a, c0 + hb] + sq[r0 + 1 - a, c0 + b])
                    + sq[r0 + a, c0 + 1 - b]
                )
                s1, s2, s3 = split3(total * -0.5)
                pick = lambda base, x: jnp.where(
                    row8 == x, s1, jnp.where(row8 == x + 1, s2, jnp.where(row8 == x + 2, s3, base[...]))
                )
                zeros8 = jnp.zeros((8, 256), F32)
                aug_r = jnp.concatenate([pick(base_r, 3), zeros8], axis=0).astype(BF16)
                aug_l = jnp.concatenate([pick(base_l, 0), zeros8], axis=0).astype(BF16)
                rhs = jnp.concatenate([opposite, vert, horiz, aug_r, hot[2 * bj + b]], axis=0)
                lhs_t = jnp.concatenate([-opposite, vert, horiz, aug_l, jnp.zeros((48, 256), BF16)], axis=0)
                weight = jnp.concatenate([wv[a], whb[2 * bi + a, b]], axis=1)
                rest = dot(jnp.concatenate([lhs_t.T, weight], axis=0), rhs)
                h = spread_ref[2 * bi + a, 2 * bj + b]
                kernel = jnp.exp2((qs[slot, 0:256] + rest[0:256]) * (2.0 * LOG2E / h))
                klow[slot, n] = kernel.astype(BF16)
                score = qs[slot, 256 + 64 * n : 320 + 64 * n] + rest[256:320]
                st[slot, n, 0:64] = score.astype(BF16)
                st[slot, n, 64:128] = own[n]

            return node

        def stage_c(k, slot):
            bi, bj = self.block_of(k)

            def node(n):
                a, b = n // 2, n % 2
                h = spread_ref[2 * bi + a, 2 * bj + b]
                scale = 2.0 / h
                prod = dot(st[slot, n], klow[slot, n])
                pull, push, colsum = prod[0:64], prod[64:128], prod[128:136]
                s = st[slot, n, 0:64].astype(F32)
                x = st[slot, n, 64:128].astype(F32)
                v = (push - x * jnp.concatenate([colsum] * 8, axis=0)) * scale
                force = pull - v
                fo[2 * bi + a, 2 * bj + b] = force.astype(BF16)
                acc[...] += row_fold(s * (force - v)) + (2.0 * scale) * row_fold(x * v) + (8.0 * scale) * colsum

            return node

        blocks = brows * bcols

        pl.semaphore_wait(barrier, n_gx + n_gy - 2)
        for off in range(1, n_gx):
            pl.semaphore_signal(
                ready, inc=1, device_id={"gx": lax.rem(gx + off, n_gx), "gy": gy}, device_id_type=MESH
            )

        @pl.when(has_down)
        def _():
            for j in v_order:
                down_copy(j).start()

        @pl.when(has_up)
        def _():
            for j in v_order:
                up_copy(j).start()

        @pl.when(has_right)
        def _():
            for i in h_order:
                right_copy(i).start()

        @pl.when(has_left)
        def _():
            for i in h_order:
                left_copy(i).start()

        for slot in range(2):
            node = stage_a(slot, slot)
            for n in range(4):
                node(n)

        unroll = 3
        steps = (blocks // 2 - 1) // unroll
        inner = (brows - 2) * (bcols - 2)

        def body(j, _):
            for step in range(steps):
                first = 2 * (unroll * step + 1)
                if first + 2 * unroll > inner:
                    pl.when(j == step)(functools.partial(arrivals, max(first, inner), first + 2 * unroll))
            for u in range(unroll):
                p = unroll * j + u
                for slot in range(2):
                    behind, ahead = stage_c(2 * p + slot, slot), stage_a(2 * p + 2 + slot, slot)
                    for n in range(4):
                        behind(n)
                        ahead(n)
            return 0

        lax.fori_loop(0, steps, body, 0)
        for slot in range(2):
            node = stage_c(blocks - 2 + slot, slot)
            for n in range(4):
                node(n)

        mine = jnp.sum(acc[:, 0:128] + acc[:, 128:256], axis=0, keepdims=True)
        me = gx * n_gy + gy
        ar_stage[0] = mine
        ar_all[me] = mine

        def ring(d, n):
            return min(d % n, n - d % n)

        def distance(off):
            z = (ring(off[0] // 2, n_gx // 2) + ring((off[0] + 1) // 2, n_gx // 2)) / 2
            y = (ring(off[1] // 4, 4) * (4 - off[1] % 4) + ring(off[1] // 4 + 1, 4) * (off[1] % 4)) / 4
            return z + y + ring(off[1], 4)

        offs = [(i, j) for i in range(n_gx) for j in range(n_gy) if i or j]
        offs.sort(key=distance, reverse=True)

        def sum_copy(t):
            i, j = offs[t]
            return pltpu.make_async_remote_copy(
                src_ref=ar_stage, dst_ref=ar_all.at[pl.ds(me, 1)], send_sem=ar_send.at[t], recv_sem=ar_recv.at[t],
                device_id={"gx": lax.rem(gx + i, n_gx), "gy": lax.rem(gy + j, n_gy)}, device_id_type=MESH,
            )

        pl.semaphore_wait(ready, n_gx - 1)
        for t in range(len(offs)):
            sum_copy(t).start()
        for t in range(len(offs)):
            sum_copy(t).wait_send()

        @pl.when(has_down)
        def _():
            for j in v_order:
                down_copy(j).wait_send()

        @pl.when(has_up)
        def _():
            for j in v_order:
                up_copy(j).wait_send()

        @pl.when(has_right)
        def _():
            for i in h_order:
                right_copy(i).wait_send()

        @pl.when(has_left)
        def _():
            for i in h_order:
                left_copy(i).wait_send()

        for t in range(len(offs)):
            sum_copy(t).wait_recv()
        pairs = float(rows * n_gx * cols * n_gy * 256 * 256)
        stein_ref[0, 0] = jnp.sum(ar_all[...]) / pairs


def solution(mesh):
    n_gx, n_gy = mesh.shape["gx"], mesh.shape["gy"]

    def step(particles, bias, spread, precision, coupling_h, coupling_v):
        rows, cols = particles.shape[:2]
        dma = pltpu.SemaphoreType.DMA
        hbm = pl.BlockSpec(memory_space=pltpu.HBM)
        smem = pl.BlockSpec(memory_space=pltpu.SMEM)
        force, stein = pl.pallas_call(
            Kernel(n_gx, n_gy, rows, cols),
            name="svgd",
            out_shape=(
                jax.ShapeDtypeStruct(particles.shape, BF16),
                jax.ShapeDtypeStruct((1, 1), F32),
            ),
            in_specs=[hbm] * 6,
            out_specs=(pl.BlockSpec(memory_space=pltpu.VMEM), smem),
            scratch_shapes=[
                pltpu.VMEM(bias.shape, F32),
                pltpu.SMEM(spread.shape, F32),
                pltpu.VMEM((64, 64), BF16),
                pltpu.VMEM((64, 64), BF16),
                pltpu.VMEM((64, 64), BF16),
                dma((5,)),
                pltpu.VMEM((rows + 2, cols + 2, 64, 256), BF16),
                pltpu.VMEM((rows + 2, cols + 2, 8, 256), F32),
                pltpu.VMEM((2, 4, 256, 256), BF16),
                pltpu.VMEM((2, 4, 144, 256), BF16),
                pltpu.VMEM((2, 512, 256), F32),
                pltpu.VMEM((cols, 48, 256), BF16),
                pltpu.VMEM((8, 256), F32),
                pltpu.VMEM((8, 256), F32),
                pltpu.VMEM((256, 256), BF16),
                pltpu.VMEM((2, 64, 128), BF16),
                pltpu.VMEM((rows, 2, 64, 128), BF16),
                pltpu.VMEM((8, 256), F32),
                pltpu.VMEM((1, 1, 128), F32),
                pltpu.VMEM((n_gx * n_gy, 1, 128), F32),
                dma((rows // 2,)),
                dma((2, rows // 2)),
                dma((2, rows // 2)),
                dma((2, cols // 2)),
                dma((2, cols // 2)),
                dma((n_gx * n_gy - 1,)),
                dma((n_gx * n_gy - 1,)),
                pltpu.SemaphoreType.REGULAR,
            ],
            compiler_params=pltpu.CompilerParams(collective_id=0, has_side_effects=True, vmem_limit_bytes=50_000_000),
        )(particles, *(pltpu.with_memory_space_constraint(v, pltpu.HBM) for v in (bias, spread, precision, coupling_h, coupling_v)))
        return force, stein[0, 0]

    return jax.shard_map(
        step,
        mesh=mesh,
        in_specs=(P("gx", "gy", None, None), P("gx", "gy", None), P("gx", "gy"), P(), P(), P()),
        out_specs=(P("gx", "gy", None, None), P()),
        check_vma=False,
    )
```
